512 devices in a mesh: seq: 32 (over z, core), mp: 4 (over x), batch: 4 (over y).
Axes of the slice: x: 4, y: 4, z: 16, core: 2. Of those that a mesh axis runs over, the one named last changes fastest.
Arguments:
- queries: bfloat16 [4, 128, 4096], P('batch', 'seq', 'mp'), may hold values from -6 to 6
- keys: bfloat16 [4, 8192, 1024], P('batch', 'seq', 'mp'), may hold values from -6 to 6
- values: bfloat16 [4, 8192, 1024], P('batch', 'seq', 'mp'), may hold values from -6 to 6
- key_position: float32 [32, 128], replicated, may hold values from -4 to 4
- compress_keys: bfloat16 [4096, 128], replicated, may hold values from -0.2 to 0.2
- compress_values: bfloat16 [4096, 128], replicated, may hold values from -0.09375 to 0.09375
- out_proj: bfloat16 [4096, 4096], P('mp', 'seq'), may hold values from -0.09375 to 0.09375
- residual: bfloat16 [4, 128, 4096], P(None, None, 'seq'), may hold values from -6 to 6
- norm_gain: float32 [4096], replicated, may hold values from 0.25 to 1.75
- lm_head: bfloat16 [131072, 4096], P(('seq', 'mp', 'batch')), may hold values from -0.4 to 0.4
- targets: int32 [4, 128], replicated, may hold values from 0 to 131071
- lengths: int32 [4], replicated, may hold values from 2048 to 8192
Outputs:
- token_logprob: float32 [4, 128], P('batch', 'seq')
- rollout_score: float32 [4], P('batch')
The draws below stay inside these ranges and needn't reach their ends.
All inputs are finite; a program needn't handle non-finite values.
Results may differ from the reference program's by a relative error of at most 0.0005.
The reference program's roundings to bfloat16 on the way count: a program that leaves them out, or rounds other values in their place, can miss the bound.
Values may be sent and summed in bfloat16 or wider, within the bound.
A program may use at most 64 MiB of HBM per device.

```python
import math
import jax
import jax.numpy as jnp
import numpy as np
from jax import lax

D = 4096
HEADS = 32
KV_HEADS = 8
HEAD_DIM = 128
BLOCK = 32
STRIDE = 16
SKIP = 64
LENGTH = 8192
SCORED = 128
NBLK = 512
ROLLOUTS = 4
VOCAB = 131072


def labelled(key, label):
    return jax.random.fold_in(key, label)


def compress_table(key):
    fan = BLOCK * HEAD_DIM
    raw = jax.random.normal(labelled(key, 101), (fan, HEAD_DIM), jnp.float32)
    return jnp.clip(raw, -4.5, 4.5) * fan ** (-0.5)


def draw_compress_keys(key, part):
    return compress_table(key).astype(jnp.bfloat16)


def draw_keys(key, part):
    shape = (ROLLOUTS, LENGTH, KV_HEADS * HEAD_DIM)
    base = jnp.clip(jax.random.normal(labelled(key, 104), shape, jnp.float32), -6.0, 6.0)
    return base.astype(jnp.bfloat16)


def draw_queries(key, part):
    shape = (ROLLOUTS, SCORED, HEADS, HEAD_DIM)
    base = jnp.clip(jax.random.normal(labelled(key, 105), shape, jnp.float32), -6.0, 6.0)
    return base.reshape(ROLLOUTS, SCORED, HEADS * HEAD_DIM).astype(jnp.bfloat16)


def draw_residual(key, part):
    shape = (ROLLOUTS, SCORED, D)
    base = jnp.clip(jax.random.normal(labelled(key, 108), shape, jnp.float32), -6.0, 6.0)
    return base.astype(jnp.bfloat16)


def draw_lm_head(key, part):
    noise = jax.random.normal(labelled(key, 111), (VOCAB, D), jnp.float32)
    base = jnp.clip(0.047 * noise, -0.28, 0.28)
    return base.astype(jnp.bfloat16)


def touch_ends(result, key, smallest, high):
    spot = [jax.random.randint(jax.random.fold_in(key, axis), (), 0, length) for axis, length in enumerate(result.shape)]
    longest = result.shape.index(max(result.shape))
    neighbour = spot[:longest] + [(spot[longest] + 1) % result.shape[longest]] + spot[longest + 1:]
    return result.at[tuple(spot)].set(smallest).at[tuple(neighbour)].set(high)


def shard_levels(key, shape, split, smallest, largest):
    level = 1.0
    for axis_at, parts in split:
        draws = jax.random.uniform(jax.random.fold_in(jax.random.fold_in(key, 6), axis_at), (parts,), jnp.float32, smallest / len(split), largest / len(split))
        level = level * jnp.repeat(jnp.exp(draws), shape[axis_at] // parts).reshape((-1,) + (1,) * (len(shape) - 1 - axis_at))
    return level


def wide_ids(own_key, dims, amount, skew):
    loads = [min(1 << octave, amount + 1 - (1 << octave)) * (1 << 20) // math.isqrt((1 << octave) ** skew) + 1 for octave in range((amount + 1).bit_length()) if 1 << octave <= amount]
    width = 1 + sum(loads) // (1 << 30)
    grid = np.cumsum(np.array([max(1, weight // width) for weight in loads]))
    pick = jax.random.randint(jax.random.fold_in(own_key, 1), dims, 0, int(grid[len(loads) - 1]))
    start = jnp.left_shift(1, jnp.searchsorted(jnp.asarray(grid, jnp.int32), pick, side="right").astype(jnp.int32))
    grade = start - 1 + jax.random.randint(jax.random.fold_in(own_key, 4), dims, 0, 1 << 30) % jnp.minimum(start, amount + 1 - start)
    return jax.random.permutation(jax.random.fold_in(own_key, 2), amount)[grade].astype(jnp.int32)


def normal_values(stream_key, dims, scale, bound, cuts=(), held_as=jnp.bfloat16):
    loudness = shard_levels(stream_key, dims, cuts, -0.22, 0.18) if cuts else 1.0
    entries = jax.random.normal(stream_key, dims, jnp.float32) * scale * loudness
    return jnp.minimum(jnp.maximum(entries, -bound), bound).astype(held_as)


def setup_inputs(seed: int = 0) -> dict:
    streams_of = jax.random.split(jax.random.key(seed), 13)
    return {
        "queries": draw_queries(jax.random.fold_in(streams_of[12], 71), 0),
        "keys": draw_keys(jax.random.fold_in(streams_of[12], 71), 0),
        "values": normal_values(streams_of[2], (ROLLOUTS, LENGTH, KV_HEADS * HEAD_DIM), 1.0, 6.0, ((0, 4), (1, 32), (2, 4))),
        "key_position": normal_values(streams_of[3], (BLOCK, HEAD_DIM), 0.7, 4.0, (), jnp.float32),
        "compress_keys": draw_compress_keys(jax.random.fold_in(streams_of[12], 71), 0),
        "compress_values": normal_values(streams_of[5], (BLOCK * HEAD_DIM, HEAD_DIM), (BLOCK * HEAD_DIM) ** -0.5, 0.09375),
        "out_proj": normal_values(streams_of[6], (HEADS * HEAD_DIM, D), (HEADS * HEAD_DIM) ** -0.5, 0.09375, ((0, 4), (1, 32))),
        "residual": draw_residual(jax.random.fold_in(streams_of[12], 71), 0),
        "norm_gain": jnp.clip(1.0 + 0.15 * jax.random.normal(streams_of[8], (D,), jnp.float32), 0.25, 1.75),
        "lm_head": draw_lm_head(jax.random.fold_in(streams_of[12], 71), 0),
        "targets": touch_ends(wide_ids(streams_of[10], (ROLLOUTS, SCORED), VOCAB, 2), jax.random.fold_in(streams_of[10], 3), 0, VOCAB - 1).astype(jnp.int32),
        "lengths": touch_ends(jax.random.randint(streams_of[11], (ROLLOUTS,), LENGTH // 4, LENGTH + 1), jax.random.fold_in(streams_of[11], 1), LENGTH // 4, LENGTH).astype(jnp.int32),
    }


def compress(rows, position, weight):
    total = rows.shape[0]
    shaped = rows.reshape(total, KV_HEADS, HEAD_DIM)
    padded = jnp.concatenate([shaped, jnp.zeros((STRIDE, KV_HEADS, HEAD_DIM), shaped.dtype)], 0)
    first = padded[:total].reshape(total // STRIDE, STRIDE, KV_HEADS, HEAD_DIM)
    second = padded[STRIDE:].reshape(total // STRIDE, STRIDE, KV_HEADS, HEAD_DIM)
    blocks = jnp.concatenate([first, second], 1)
    blocks = (blocks.astype(jnp.float32) + position[None, :, None, :]).astype(jnp.bfloat16)
    mapped = jnp.einsum('bjhd,jde->bhe', blocks.astype(jnp.float32), weight.reshape(BLOCK, HEAD_DIM, HEAD_DIM).astype(jnp.float32))
    return mapped.astype(jnp.bfloat16)

def score_rollout(query_rows, key_rows, value_rows, residual_rows, target_rows, key_position, compress_keys, compress_values, out_proj, norm_gain, lm_head):
    ckey = compress(key_rows, key_position, compress_keys)
    cvalue = compress(value_rows, key_position, compress_values)
    group = HEADS // KV_HEADS
    query = query_rows.reshape(SCORED, KV_HEADS, group, HEAD_DIM).astype(jnp.float32)
    scores = jnp.einsum('qhgd,bhd->qhgb', query, ckey.astype(jnp.float32)) * (1.0 / math.sqrt(HEAD_DIM))
    limit = jnp.arange(SCORED, dtype=jnp.int32) * SKIP // STRIDE
    visible = (jnp.arange(NBLK, dtype=jnp.int32)[None, :] <= limit[:, None])[:, None, None, :]
    scores = jnp.where(visible, scores, -1e+30)
    peak = lax.optimization_barrier(jnp.max(scores, -1, keepdims=True))
    weights = jnp.where(visible, jnp.exp(scores - peak), 0.0)
    probs = (weights / lax.optimization_barrier(jnp.sum(weights, -1, keepdims=True))).astype(jnp.bfloat16)
    attended = jnp.einsum('qhgb,bhd->qhgd', probs.astype(jnp.float32), cvalue.astype(jnp.float32))
    attended = attended.astype(jnp.bfloat16).reshape(SCORED, HEADS * HEAD_DIM)
    hidden = (residual_rows.astype(jnp.float32) + jnp.dot(attended, out_proj, preferred_element_type=jnp.float32)).astype(jnp.bfloat16)
    widened = hidden.astype(jnp.float32)
    meansq = lax.optimization_barrier(jnp.mean(widened * widened, -1, keepdims=True))
    normed = (widened * lax.rsqrt(meansq + 1e-05) * norm_gain).astype(jnp.bfloat16)
    logits = jnp.dot(normed, lm_head.T, preferred_element_type=jnp.float32)
    top = lax.optimization_barrier(jnp.max(logits, -1, keepdims=True))
    logsum = top[:, 0] + jnp.log(lax.optimization_barrier(jnp.sum(jnp.exp(logits - top), -1)))
    picked = jnp.take_along_axis(logits, target_rows[:, None], 1)[:, 0]
    return picked - logsum

def reference(queries, keys, values, key_position, compress_keys, compress_values, out_proj, residual, norm_gain, lm_head, targets, lengths):

    def one(items):
        return score_rollout(items[0], items[1], items[2], items[3], items[4], key_position, compress_keys, compress_values, out_proj, norm_gain, lm_head)
    token_logprob = lax.map(one, (queries, keys, values, residual, targets))
    spots = jnp.arange(SCORED, dtype=jnp.int32) * SKIP + BLOCK - 1
    valid = (spots[None, :] < lengths[:, None]).astype(jnp.float32)
    count = jnp.sum(valid)
    rollout_score = lax.optimization_barrier(jnp.sum(valid * token_logprob, 1)) / count
    return (token_logprob, rollout_score)
```

```python
import functools
import math

import jax
import jax.numpy as jnp
from jax import lax
from jax.experimental import pallas as pl
from jax.experimental.pallas import tpu as pltpu
from jax.sharding import Mesh
from jax.sharding import PartitionSpec as P

BF16 = jnp.bfloat16
F32 = jnp.float32
HEAD_DIM = 128
MESH = pl.DeviceIdType.MESH
AXES = ("seq_0", "seq_1", "mp", "batch")
SEQ = ("seq_0", "seq_1")
SEQ_MP_BATCH = ("seq_0", "seq_1", "mp", "batch")
NZ, NX, NY = 16, 4, 4

SHIFT = (0, 1, 2, -1, -2)
STEP = (0, 5, -5)
OFFSETS = tuple(s + w for s in SHIFT for w in STEP) + (8,)
SLOT_OF = {off % NZ: k for k, off in enumerate(OFFSETS)}
NEAR = (0, 1, -1, 2, -2, 3, -3, 4, -4, 5, -5, 6, -6, 7, -7, 8)
CHUNK = 4
CHUNKS = NZ // CHUNK


def nt_dot(a, b):
    return lax.dot_general(a, b, (((1,), (1,)), ((), ())), preferred_element_type=F32)


def kernel(
    q_ref, k_ref, v_ref, pos_ref, wk_hbm, wv_hbm, op_hbm, res_ref, gain_ref, lm_hbm, tgt_ref, len_ref,
    out_ref,
    w_buf, op_own, op_other, lm_buf, rows_f, xa, xb, pay, epay, bz, kvq, ebuf, qperm, kmat, vmat, att,
    cs, cr, g_own, g_other, rb, normed, acc, st, fr, fs, zr,
    local_sem, b_send, b_recv, a1_send, a1_recv, a2_send, a2_recv, c_send, c_recv, d1_send, d1_recv,
    d2_send, d2_recv, d3_send, d3_recv, d4_send, d4_recv, f1_send, f1_recv, f2_send, f2_recv,
):
    z, c, x, y = (lax.axis_index(name) for name in AXES)
    other = 1 - c

    def at_z(off):
        return lax.rem(z + (off + NZ), NZ)

    def ring4(p, d):
        return lax.rem(p + d, 4)

    barrier = pltpu.get_barrier_semaphore()
    peers = [(at_z(off), core, x, y) for off in range(1, NZ) for core in (0, 1)]
    peers += [(z, other, ring4(x, d), y) for d in range(4)]
    peers += [(z, c, ring4(x, d), ring4(y, e)) for d in range(4) for e in range(4) if d or e]
    for peer in peers:
        pl.semaphore_signal(barrier, inc=1, device_id=peer, device_id_type=MESH)

    loads = [
        pltpu.make_async_copy(wk_hbm, w_buf.at[0], local_sem.at[0]),
        pltpu.make_async_copy(wv_hbm, w_buf.at[1], local_sem.at[1]),
        pltpu.make_async_copy(op_hbm.at[pl.ds(pl.multiple_of(c * 512, 512), 512)], op_own, local_sem.at[2]),
        pltpu.make_async_copy(lm_hbm, lm_buf.at[c], local_sem.at[3]),
    ]
    for load in loads:
        load.start()

    for t, src in enumerate((k_ref, v_ref)):
        for h in range(2):
            rows_f[t, h] = src[0, :, h * 128 : (h + 1) * 128].astype(F32)
    for i in range(16):
        lanes = slice(i * 128, (i + 1) * 128)
        pa, pb = pos_ref[i : i + 1, :], pos_ref[16 + i : 17 + i, :]
        for t in range(2):
            for h in range(2):
                rows = rows_f[t, h, pl.ds(i, 16, stride=16), :]
                xa[t, h * 16 : (h + 1) * 16, lanes] = (rows + pa).astype(BF16)
                xb[t, h * 16 : (h + 1) * 16, lanes] = (rows + pb).astype(BF16)
            xb[t, 32:48, lanes] = jnp.broadcast_to(pb, (16, 128)).astype(BF16)
    qf = q_ref[0].astype(F32)
    for h in range(2):
        lines = [qf[:, (4 * h + g) * 128 : (4 * h + g + 1) * 128] for g in range(4)]
        pay[h, 2] = jnp.concatenate(lines, 0).astype(BF16)
    for t in range(2):
        loads[t].wait()
        first = jnp.dot(xa[t], w_buf[t, :2048], preferred_element_type=F32)
        second = jnp.dot(xb[t], w_buf[t, 2048:], preferred_element_type=F32)
        bz[t] = second[32:33]
        for h in range(2):
            fh, sh = first[h * 16 : (h + 1) * 16], second[h * 16 : (h + 1) * 16]
            pay[h, t] = (fh + pltpu.roll(sh, 15, 0)).astype(BF16)
            epay[h, 2 * t : 2 * t + 1] = fh[15:16]
            epay[h, 2 * t + 1 : 2 * t + 2] = sh[0:1]
    kvq[0, c] = pay[c]
    ebuf[0, c] = epay[c]

    pl.semaphore_wait(barrier, len(peers))

    def remote(src, dst, send, recv, peer):
        return pltpu.make_async_remote_copy(
            src_ref=src, dst_ref=dst, send_sem=send, recv_sem=recv, device_id=peer, device_id_type=MESH
        )

    sent = []

    def go(copy):
        copy.start()
        sent.append(copy)

    def a1(n, k, core, h):
        peer = (at_z(-OFFSETS[k]), core, x, y)
        i = 3 * n + (2 if k == 15 else k - 1) if k else 6
        return (
            remote(pay.at[h], kvq.at[k, c], a1_send.at[2 * i], a1_recv.at[4 * (3 if k == 15 else k) + 2 * c], peer),
            remote(epay.at[h], ebuf.at[k, c], a1_send.at[2 * i + 1], a1_recv.at[4 * (3 if k == 15 else k) + 2 * c + 1], peer),
        )

    for k in (15, 1, 2):
        for n, h in enumerate((c, other)):
            for part in a1(n, k, h, h):
                go(part)
    for part in a1(0, 0, other, other):
        go(part)

    op_copy = remote(op_hbm.at[pl.ds(pl.multiple_of(other * 512, 512), 512)], op_other, b_send.at[0], b_recv.at[0], (z, other, x, y))
    lm_copy = remote(lm_hbm, lm_buf.at[c], b_send.at[1], b_recv.at[1], (z, other, x, y))
    go(op_copy)
    go(lm_copy)

    def a1_arrival(k, core):
        i = 4 * (3 if k == 15 else k) + 2 * core
        remote(pay.at[0], kvq.at[k, core], a1_send.at[0], a1_recv.at[i], (z, c, x, y)).wait_recv()
        remote(epay.at[0], ebuf.at[k, core], a1_send.at[0], a1_recv.at[i + 1], (z, c, x, y)).wait_recv()

    a1_arrival(0, other)
    for k in (1, 2):
        for core in range(2):
            a1_arrival(k, core)

    def a2(g):
        peer = (at_z(-SHIFT[g]), c, x, y)
        return (
            remote(kvq.at[pl.ds(0, 3)], kvq.at[pl.ds(3 * g, 3)], a2_send.at[2 * g - 2], a2_recv.at[2 * g - 2], peer),
            remote(ebuf.at[pl.ds(0, 3)], ebuf.at[pl.ds(3 * g, 3)], a2_send.at[2 * g - 1], a2_recv.at[2 * g - 1], peer),
        )

    for g in (2, 4, 1, 3):
        for part in a2(g):
            go(part)

    col = lax.broadcasted_iota(jnp.int32, (1, 512), 1)
    slot, core_of, lane = col // 32, (col // 16) % 2, col % 16
    g_of, w_of = slot // 3, slot % 3
    off_of = jnp.where(g_of > 2, 2 - g_of, g_of) + jnp.where(w_of == 2, -5, 5 * w_of)
    off_of = jnp.where(slot == 15, 8, off_of)
    seq_of = ((off_of + z + NZ) % NZ) * 2 + core_of
    block_of = seq_of * 16 + lane
    row_of = (lane // 4) * 128 + seq_of * 4 + lane % 4
    perm = jnp.where(lax.broadcasted_iota(jnp.int32, (512, 512), 0) == row_of, 1.0, 0.0).astype(BF16)

    for core in range(2):
        a1_arrival(15, core)
    for g in (1, 3, 2, 4):
        for part in a2(g):
            part.wait_recv()

    q_all = kvq[:, :, 2].reshape(512, 128)
    qperm[...] = jnp.dot(perm, q_all, preferred_element_type=F32).astype(BF16)
    last = lax.broadcasted_iota(jnp.int32, (16, 128), 0) == 15
    for k in range(NZ):
        top = (at_z(OFFSETS[k]) == NZ - 1).astype(F32)
        after = SLOT_OF[(OFFSETS[k] + 1) % NZ]
        for t, mat in enumerate((kmat, vmat)):
            for core in range(2):
                if core == 0:
                    beyond = ebuf[k, 1, 2 * t + 1 : 2 * t + 2]
                else:
                    beyond = ebuf[after, 0, 2 * t + 1 : 2 * t + 2] * (1.0 - top) + bz[t] * top
                fixed = ebuf[k, core, 2 * t : 2 * t + 1] + beyond
                tile = jnp.where(last, fixed, kvq[k, core, t].astype(F32))
                mat[(2 * k + core) * 16 : (2 * k + core + 1) * 16, :] = tile.astype(BF16)

    limit = lax.broadcasted_iota(jnp.int32, (128, 1), 0) * 4
    visible = block_of <= limit
    for g in range(4):
        score = nt_dot(qperm[g * 128 : (g + 1) * 128], kmat[...]) * (1.0 / math.sqrt(HEAD_DIM))
        score = jnp.where(visible, score, -1e30)
        peak = jnp.max(score, -1, keepdims=True)
        weight = jnp.where(visible, jnp.exp(score - peak), 0.0)
        prob = (weight * (1.0 / jnp.sum(weight, -1, keepdims=True))).astype(BF16)
        found = jnp.dot(prob, vmat[...], preferred_element_type=F32)
        att[:, g * 128 : (g + 1) * 128] = found.astype(BF16)

    loads[2].wait()
    cs[0] = jnp.dot(att[...], op_own[...], preferred_element_type=F32).reshape(4, 32, 128)
    op_copy.wait_recv()
    cs[1] = jnp.dot(att[...], op_other[...], preferred_element_type=F32).reshape(4, 32, 128)

    def c_copy(rel, d):
        to = ring4(x, d)
        i = rel * 4 + d
        return remote(cs.at[rel, to], cr.at[i], c_send.at[i], c_recv.at[i], (z, other if rel else c, to, y))

    pairs = [(rel, d) for d in (2, 1, 3, 0) for rel in (0, 1) if rel or d]
    for rel, d in pairs:
        go(c_copy(rel, d))
    total = res_ref[y, pl.ds(pl.multiple_of(32 * x, 32), 32), :].astype(F32)
    summed = cs[0, x]
    for rel, d in reversed(pairs):
        c_copy(rel, d).wait_recv()
        summed = summed + cr[rel * 4 + d]
    p1 = x * other + y * c
    p2 = x * c + y * other
    g_own[p2, p1, 0] = (total + summed).astype(BF16)

    def d1(o):
        return remote(g_own.at[p2, p1, 0], g_own.at[p2, p1, o], d1_send.at[o], d1_recv.at[o], (at_z(-NEAR[o]), c, x, y))

    for o in reversed(range(1, NZ)):
        go(d1(o))

    def along_first(d):
        return (z, c, ring4(x, d * other), ring4(y, d * c))

    def along_second(d):
        return (z, c, ring4(x, d * c), ring4(y, d * other))

    def d2(s, d):
        part = pl.ds(s * CHUNK, CHUNK)
        i = s * 3 + d - 1
        return remote(g_own.at[p2, p1, part], g_own.at[p2, p1, part], d2_send.at[i], d2_recv.at[i], along_first(d))

    def d2_arrival(s, d):
        part = pl.ds(s * CHUNK, CHUNK)
        i = s * 3 + d - 1
        slab = g_own.at[p2, ring4(p1, 4 - d), part]
        remote(slab, slab, d2_send.at[i], d2_recv.at[i], along_first(d)).wait_recv()

    def d3(s, e, d):
        part = pl.ds(s * CHUNK, CHUNK)
        i = (s * 4 + e) * 3 + d - 1
        slab = g_own.at[p2, ring4(p1, 4 - e), part]
        return remote(slab, slab, d3_send.at[i], d3_recv.at[i], along_second(d))

    def d3_arrival(s, e, d):
        part = pl.ds(s * CHUNK, CHUNK)
        i = (s * 4 + e) * 3 + d - 1
        slab = g_own.at[ring4(p2, 4 - d), ring4(p1, 4 - e), part]
        remote(slab, slab, d3_send.at[i], d3_recv.at[i], along_second(d)).wait_recv()

    for s in range(CHUNKS):
        for o in range(max(1, s * CHUNK), (s + 1) * CHUNK):
            d1(o).wait_recv()
        for d in (2, 1, 3):
            go(d2(s, d))
        for d in (2, 1, 3):
            go(d3(s, 0, d))
    for s in range(CHUNKS):
        for e in (1, 3, 2):
            d2_arrival(s, e)
            for d in (2, 1, 3):
                go(d3(s, e, d))
    for s in range(CHUNKS):
        for e in (0, 1, 3, 2):
            for d in (1, 3, 2):
                d3_arrival(s, e, d)

    def held(core_rows, parity, n):
        xx, yy = n % 4, 2 * core_rows + n // 4
        return xx * parity + yy * (1 - parity), xx * (1 - parity) + yy * parity

    def d4(n):
        i, j = held(other, c, n)
        return remote(g_own.at[i, j], g_other.at[i, j], d4_send.at[n], d4_recv.at[n], (z, other, x, y))

    for n in range(8):
        go(d4(n))

    def squares(ref, i, j):
        part = ref[i, j].astype(F32)
        return jnp.sum(part * part, 0)

    for n in range(8):
        i, j = held(c, c, n)
        rb[n] = squares(g_own, i, j)
    for n in range(8):
        i, j = held(c, other, n)
        remote(g_other.at[i, j], g_other.at[i, j], d4_send.at[n], d4_recv.at[n], (z, other, x, y)).wait_recv()
        total_sq = jnp.sum(rb[n] + squares(g_other, i, j), -1, keepdims=True)
        rb[n] = jnp.broadcast_to(lax.rsqrt(total_sq * (1.0 / 4096) + 1e-05), (32, 128))

    loads[3].wait()
    lm_copy_in = remote(lm_hbm, lm_buf.at[other], b_send.at[1], b_recv.at[1], (z, other, x, y))
    lm_copy_in.wait_recv()
    for o in range(NZ):
        for ref, parity in ((g_own, c), (g_other, other)):
            at = pl.multiple_of((at_z(NEAR[o]) * 2 + parity) * 128, 128)
            gain = gain_ref[:, pl.ds(at, 128)]
            for n in range(8):
                i, j = held(c, parity, n)
                normed[n * 32 : (n + 1) * 32, pl.ds(at, 128)] = (ref[i, j, o].astype(F32) * rb[n] * gain).astype(BF16)

    for half in range(2):
        acc[half] = nt_dot(lm_buf[half, :, :512], normed[:, :512])

    @pl.loop(1, 8)
    def _(t):
        lanes = pl.ds(pl.multiple_of(t * 512, 512), 512)
        for half in range(2):
            acc[half] += nt_dot(lm_buf[half, :, lanes], normed[:, lanes])

    logits = [acc[0], acc[1]]
    peak = jnp.maximum(jnp.max(logits[0], 0, keepdims=True), jnp.max(logits[1], 0, keepdims=True))
    wanted = jnp.concatenate([tgt_ref[pl.ds(2 * c, 1), :], tgt_ref[pl.ds(2 * c + 1, 1), :]], 1)
    spread = jnp.zeros((1, 256), F32)
    picked = jnp.zeros((1, 256), F32)
    for half in range(2):
        base = (((2 * z + half) * NX + x) * NY + y) * 256
        entry = base + lax.broadcasted_iota(jnp.int32, (256, 256), 0)
        spread += jnp.sum(jnp.exp(logits[half] - peak), 0, keepdims=True)
        picked += jnp.sum(jnp.where(entry == wanted, logits[half], 0.0), 0, keepdims=True)
    partial = peak + jnp.log(spread)
    for n in range(2):
        st[n, 0:1] = partial[:, n * 128 : (n + 1) * 128]
        st[n, 1:2] = picked[:, n * 128 : (n + 1) * 128]

    active = c == y // 2

    def f1(n, d, e):
        i = d * 4 + e
        return remote(st.at[n], fr.at[x * 4 + y], f1_send.at[n * 4 + d], f1_recv.at[i], (z, c, ring4(x, d), 2 * c + n))

    for n in range(2):
        e = lax.rem(2 * c + n - y + 4, 4)
        for d in (2, 1, 3):
            f1(n, d, e).start()

        @pl.when(e != 0)
        def _():
            f1(n, 0, e).start()

        @pl.when(e == 0)
        def _():
            fr[x * 4 + y] = st[n]

    def joined(ref):
        heads = [ref[n] for n in range(16)]
        high = functools.reduce(jnp.maximum, [part[0:1] for part in heads])
        mass = functools.reduce(jnp.add, [jnp.exp(part[0:1] - high) for part in heads])
        return high + jnp.log(mass), functools.reduce(jnp.add, [part[1:2] for part in heads])

    def f2(o, core, n):
        return remote(fs, zr.at[o], f2_send.at[2 * o + n], f2_recv.at[o], (at_z(-NEAR[o]), core, x, y))

    @pl.when(active)
    def _():
        for d in range(4):
            for e in range(4):
                if d or e:
                    here = fr.at[lax.rem(x + 4 - d, 4) * 4 + lax.rem(y + 4 - e, 4)]
                    remote(st.at[0], here, f1_send.at[0], f1_recv.at[d * 4 + e], (z, c, x, y)).wait_recv()
        level, hit = joined(fr)
        fs[0:1] = level
        fs[1:2] = hit
        for o in reversed(range(1, NZ)):
            f2(o, c, 0).start()
            f2(o, other, 1).start()
        f2(0, other, 1).start()
        zr[0] = fs[...]

    for o in range(1, NZ):
        f2(o, c, 0).wait_recv()

    @pl.when(jnp.logical_not(active))
    def _():
        f2(0, other, 1).wait_recv()

    level, hit = joined(zr)
    logprob = hit - level
    spots = lax.broadcasted_iota(jnp.int32, (1, 128), 1) * 64 + 31
    count = jnp.zeros((1, 1), F32)
    for n in range(4):
        count += jnp.sum(jnp.where(spots < len_ref[n], 1.0, 0.0), -1, keepdims=True)
    mine = jnp.where(spots < len_ref[y], 1.0, 0.0)
    score = jnp.sum(mine * logprob, -1, keepdims=True) / count
    out_ref[0:1] = logprob
    out_ref[1:2] = jnp.broadcast_to(score, (1, 128))

    for copy in sent:
        copy.wait_send()
    for n in range(2):
        e = lax.rem(2 * c + n - y + 4, 4)
        for d in (2, 1, 3):
            f1(n, d, e).wait_send()

        @pl.when(e != 0)
        def _():
            f1(n, 0, e).wait_send()

    @pl.when(active)
    def _():
        for o in reversed(range(1, NZ)):
            f2(o, c, 0).wait_send()
            f2(o, other, 1).wait_send()
        f2(0, other, 1).wait_send()


def body(
    queries, keys, values, key_position, compress_keys, compress_values,
    out_proj, residual, norm_gain, lm_head, targets, lengths,
):
    vmem = pl.BlockSpec(memory_space=pltpu.VMEM)
    hbm = pl.BlockSpec(memory_space=pl.ANY)
    smem = pl.BlockSpec(memory_space=pltpu.SMEM)
    dma = pltpu.SemaphoreType.DMA
    found = pl.pallas_call(
        kernel,
        out_shape=jax.ShapeDtypeStruct((2, 128), F32),
        in_specs=[vmem, vmem, vmem, vmem, hbm, hbm, hbm, vmem, vmem, hbm, vmem, smem],
        out_specs=vmem,
        scratch_shapes=[
            pltpu.VMEM((2, 4096, 128), BF16),
            pltpu.VMEM((512, 128), BF16),
            pltpu.VMEM((512, 128), BF16),
            pltpu.VMEM((2, 256, 4096), BF16),
            pltpu.VMEM((2, 2, 256, 128), F32),
            pltpu.VMEM((2, 32, 2048), BF16),
            pltpu.VMEM((2, 48, 2048), BF16),
            pltpu.VMEM((2, 3, 16, 128), BF16),
            pltpu.VMEM((2, 4, 128), F32),
            pltpu.VMEM((2, 1, 128), F32),
            pltpu.VMEM((16, 2, 3, 16, 128), BF16),
            pltpu.VMEM((16, 2, 4, 128), F32),
            pltpu.VMEM((512, 128), BF16),
            pltpu.VMEM((512, 128), BF16),
            pltpu.VMEM((512, 128), BF16),
            pltpu.VMEM((128, 512), BF16),
            pltpu.VMEM((2, 4, 32, 128), F32),
            pltpu.VMEM((8, 32, 128), F32),
            pltpu.VMEM((4, 4, 16, 32, 128), BF16),
            pltpu.VMEM((4, 4, 16, 32, 128), BF16),
            pltpu.VMEM((8, 32, 128), F32),
            pltpu.VMEM((256, 4096), BF16),
            pltpu.VMEM((2, 256, 256), F32),
            pltpu.VMEM((2, 2, 128), F32),
            pltpu.VMEM((16, 2, 128), F32),
            pltpu.VMEM((2, 128), F32),
            pltpu.VMEM((16, 2, 128), F32),
            dma((4,)),
            dma((2,)), dma((2,)),
            dma((14,)), dma((16,)),
            dma((8,)), dma((8,)),
            dma((8,)), dma((8,)),
            dma((16,)), dma((16,)),
            dma((12,)), dma((12,)),
            dma((48,)), dma((48,)),
            dma((8,)), dma((8,)),
            dma((8,)), dma((16,)),
            dma((32,)), dma((16,)),
        ],
        compiler_params=pltpu.CompilerParams(
            collective_id=0, has_side_effects=True, vmem_limit_bytes=48 * 1024 * 1024
        ),
    )(
        queries, keys, values, key_position, compress_keys, compress_values,
        out_proj, residual, norm_gain.reshape(1, -1), lm_head, targets, lengths,
    )
    seq_pos = lax.axis_index(SEQ)
    token_logprob = lax.dynamic_slice(found, (0, seq_pos * 4), (1, 4))
    return token_logprob, found[1, :1]


def solution(mesh):
    split = Mesh(
        mesh.devices.reshape(16, 2, mesh.shape["mp"], mesh.shape["batch"]),
        ("seq_0", "seq_1", "mp", "batch"),
    )
    in_specs = (
        P("batch", SEQ, "mp"),
        P("batch", SEQ, "mp"),
        P("batch", SEQ, "mp"),
        P(),
        P(),
        P(),
        P("mp", SEQ),
        P(None, None, SEQ),
        P(),
        P(SEQ_MP_BATCH, None),
        P(),
        P(),
    )
    out_specs = (P("batch", SEQ), P("batch"))
    return jax.shard_map(body, mesh=split, in_specs=in_specs, out_specs=out_specs, check_vma=False)
```

```python
import functools
import math

import jax
import jax.numpy as jnp
from jax import lax
from jax.experimental import pallas as pl
from jax.experimental.pallas import tpu as pltpu
from jax.sharding import Mesh
from jax.sharding import PartitionSpec as P

BF16 = jnp.bfloat16
F32 = jnp.float32
HEAD_DIM = 128
MESH = pl.DeviceIdType.MESH
AXES = ("seq_0", "seq_1", "mp", "batch")
SEQ = ("seq_0", "seq_1")
SEQ_MP_BATCH = ("seq_0", "seq_1", "mp", "batch")
NZ, NX, NY = 16, 4, 4

SHIFT = (0, 1, 2, -1, -2)
STEP = (0, 5, -5)
OFFSETS = tuple(s + w for s in SHIFT for w in STEP) + (8,)
SLOT_OF = {off % NZ: k for k, off in enumerate(OFFSETS)}
NEAR = (0, 1, -1, 2, -2, 3, -3, 4, -4, 5, -5, 6, -6, 7, -7, 8)
CHUNK = 4
CHUNKS = NZ // CHUNK


def nt_dot(a, b):
    return lax.dot_general(a, b, (((1,), (1,)), ((), ())), preferred_element_type=F32)


def kernel(
    q_hbm, k_hbm, v_hbm, pos_hbm, wk_hbm, wv_hbm, op_hbm, res_hbm, gain_hbm, lm_hbm, tgt_hbm, len_hbm,
    out_ref,
    q_ref, k_ref, v_ref, pos_ref, res_ref, gain_ref, tgt_ref, len_ref, w_buf, op_own, op_other, lm_buf, rows_f, xa, xb, pay, epay, bz, kvq, ebuf, qperm, kmat, vmat, att,
    cs, cr, g_own, g_other, rb, normed, acc, st, fr, fs, zr,
    local_sem, small_sem, b_send, b_recv, a1_send, a1_recv, a2_send, a2_recv, c_send, c_recv, d1_send, d1_recv,
    d2_send, d2_recv, d3_send, d3_recv, d4_send, d4_recv, f1_send, f1_recv, f2_send, f2_recv,
):
    z, c, x, y = (lax.axis_index(name) for name in AXES)
    other = 1 - c

    def at_z(off):
        return lax.rem(z + (off + NZ), NZ)

    def ring4(p, d):
        return lax.rem(p + d, 4)

    barrier = pltpu.get_barrier_semaphore()
    peers = [(at_z(off), core, x, y) for off in range(1, NZ) for core in (0, 1)]
    peers += [(z, other, ring4(x, d), y) for d in range(4)]
    peers += [(z, c, ring4(x, d), ring4(y, e)) for d in range(4) for e in range(4) if d or e]
    for peer in peers:
        pl.semaphore_signal(barrier, inc=1, device_id=peer, device_id_type=MESH)

    loads = [
        pltpu.make_async_copy(wk_hbm, w_buf.at[0], local_sem.at[0]),
        pltpu.make_async_copy(wv_hbm, w_buf.at[1], local_sem.at[1]),
        pltpu.make_async_copy(op_hbm.at[pl.ds(pl.multiple_of(c * 512, 512), 512)], op_own, local_sem.at[2]),
        pltpu.make_async_copy(lm_hbm, lm_buf.at[c], local_sem.at[3]),
    ]
    small = [
        pltpu.make_async_copy(src, dst, small_sem.at[n])
        for n, (src, dst) in enumerate((
            (k_hbm, k_ref), (v_hbm, v_ref), (pos_hbm, pos_ref), (q_hbm, q_ref),
            (res_hbm, res_ref), (gain_hbm, gain_ref), (tgt_hbm, tgt_ref), (len_hbm, len_ref),
        ))
    ]
    for load in small[:4] + loads + small[4:]:
        load.start()
    for load in small[:4]:
        load.wait()

    for t, src in enumerate((k_ref, v_ref)):
        for h in range(2):
            rows_f[t, h] = src[0, :, h * 128 : (h + 1) * 128].astype(F32)
    for i in range(16):
        lanes = slice(i * 128, (i + 1) * 128)
        pa, pb = pos_ref[i : i + 1, :], pos_ref[16 + i : 17 + i, :]
        for t in range(2):
            for h in range(2):
                rows = rows_f[t, h, pl.ds(i, 16, stride=16), :]
                xa[t, h * 16 : (h + 1) * 16, lanes] = (rows + pa).astype(BF16)
                xb[t, h * 16 : (h + 1) * 16, lanes] = (rows + pb).astype(BF16)
            xb[t, 32:48, lanes] = jnp.broadcast_to(pb, (16, 128)).astype(BF16)
    qf = q_ref[0].astype(F32)
    for h in range(2):
        lines = [qf[:, (4 * h + g) * 128 : (4 * h + g + 1) * 128] for g in range(4)]
        pay[h, 2] = jnp.concatenate(lines, 0).astype(BF16)
    for t in range(2):
        loads[t].wait()
        first = jnp.dot(xa[t], w_buf[t, :2048], preferred_element_type=F32)
        second = jnp.dot(xb[t], w_buf[t, 2048:], preferred_element_type=F32)
        bz[t] = second[32:33]
        for h in range(2):
            fh, sh = first[h * 16 : (h + 1) * 16], second[h * 16 : (h + 1) * 16]
            pay[h, t] = (fh + pltpu.roll(sh, 15, 0)).astype(BF16)
            epay[h, 2 * t : 2 * t + 1] = fh[15:16]
            epay[h, 2 * t + 1 : 2 * t + 2] = sh[0:1]
    kvq[0, c] = pay[c]
    ebuf[0, c] = epay[c]

    pl.semaphore_wait(barrier, len(peers))

    def remote(src, dst, send, recv, peer):
        return pltpu.make_async_remote_copy(
            src_ref=src, dst_ref=dst, send_sem=send, recv_sem=recv, device_id=peer, device_id_type=MESH
        )

    sent = []

    def go(copy):
        copy.start()
        sent.append(copy)

    def a1(n, k, core, h):
        peer = (at_z(-OFFSETS[k]), core, x, y)
        i = 3 * n + (2 if k == 15 else k - 1) if k else 6
        return (
            remote(pay.at[h], kvq.at[k, c], a1_send.at[2 * i], a1_recv.at[4 * (3 if k == 15 else k) + 2 * c], peer),
            remote(epay.at[h], ebuf.at[k, c], a1_send.at[2 * i + 1], a1_recv.at[4 * (3 if k == 15 else k) + 2 * c + 1], peer),
        )

    for k in (15, 1, 2):
        for n, h in enumerate((c, other)):
            for part in a1(n, k, h, h):
                go(part)
    for part in a1(0, 0, other, other):
        go(part)

    op_copy = remote(op_hbm.at[pl.ds(pl.multiple_of(other * 512, 512), 512)], op_other, b_send.at[0], b_recv.at[0], (z, other, x, y))
    lm_copy = remote(lm_hbm, lm_buf.at[c], b_send.at[1], b_recv.at[1], (z, other, x, y))
    go(op_copy)
    go(lm_copy)

    def a1_arrival(k, core):
        i = 4 * (3 if k == 15 else k) + 2 * core
        remote(pay.at[0], kvq.at[k, core], a1_send.at[0], a1_recv.at[i], (z, c, x, y)).wait_recv()
        remote(epay.at[0], ebuf.at[k, core], a1_send.at[0], a1_recv.at[i + 1], (z, c, x, y)).wait_recv()

    a1_arrival(0, other)
    for k in (1, 2):
        for core in range(2):
            a1_arrival(k, core)

    def a2(g):
        peer = (at_z(-SHIFT[g]), c, x, y)
        return (
            remote(kvq.at[pl.ds(0, 3)], kvq.at[pl.ds(3 * g, 3)], a2_send.at[2 * g - 2], a2_recv.at[2 * g - 2], peer),
            remote(ebuf.at[pl.ds(0, 3)], ebuf.at[pl.ds(3 * g, 3)], a2_send.at[2 * g - 1], a2_recv.at[2 * g - 1], peer),
        )

    for g in (2, 4, 1, 3):
        for part in a2(g):
            go(part)

    col = lax.broadcasted_iota(jnp.int32, (1, 512), 1)
    slot, core_of, lane = col // 32, (col // 16) % 2, col % 16
    g_of, w_of = slot // 3, slot % 3
    off_of = jnp.where(g_of > 2, 2 - g_of, g_of) + jnp.where(w_of == 2, -5, 5 * w_of)
    off_of = jnp.where(slot == 15, 8, off_of)
    seq_of = ((off_of + z + NZ) % NZ) * 2 + core_of
    block_of = seq_of * 16 + lane
    row_of = (lane // 4) * 128 + seq_of * 4 + lane % 4
    perm = jnp.where(lax.broadcasted_iota(jnp.int32, (512, 512), 0) == row_of, 1.0, 0.0).astype(BF16)

    for core in range(2):
        a1_arrival(15, core)
    for g in (1, 3, 2, 4):
        for part in a2(g):
            part.wait_recv()

    q_all = kvq[:, :, 2].reshape(512, 128)
    qperm[...] = jnp.dot(perm, q_all, preferred_element_type=F32).astype(BF16)
    last = lax.broadcasted_iota(jnp.int32, (16, 128), 0) == 15
    for k in range(NZ):
        top = (at_z(OFFSETS[k]) == NZ - 1).astype(F32)
        after = SLOT_OF[(OFFSETS[k] + 1) % NZ]
        for t, mat in enumerate((kmat, vmat)):
            for core in range(2):
                if core == 0:
                    beyond = ebuf[k, 1, 2 * t + 1 : 2 * t + 2]
                else:
                    beyond = ebuf[after, 0, 2 * t + 1 : 2 * t + 2] * (1.0 - top) + bz[t] * top
                fixed = ebuf[k, core, 2 * t : 2 * t + 1] + beyond
                tile = jnp.where(last, fixed, kvq[k, core, t].astype(F32))
                mat[(2 * k + core) * 16 : (2 * k + core + 1) * 16, :] = tile.astype(BF16)

    limit = lax.broadcasted_iota(jnp.int32, (128, 1), 0) * 4
    visible = block_of <= limit
    for g in range(4):
        score = nt_dot(qperm[g * 128 : (g + 1) * 128], kmat[...]) * (1.0 / math.sqrt(HEAD_DIM))
        score = jnp.where(visible, score, -1e30)
        peak = jnp.max(score, -1, keepdims=True)
        weight = jnp.where(visible, jnp.exp(score - peak), 0.0)
        prob = (weight * (1.0 / jnp.sum(weight, -1, keepdims=True))).astype(BF16)
        found = jnp.dot(prob, vmat[...], preferred_element_type=F32)
        att[:, g * 128 : (g + 1) * 128] = found.astype(BF16)

    loads[2].wait()
    cs[0] = jnp.dot(att[...], op_own[...], preferred_element_type=F32).reshape(4, 32, 128)
    op_copy.wait_recv()
    cs[1] = jnp.dot(att[...], op_other[...], preferred_element_type=F32).reshape(4, 32, 128)

    def c_copy(rel, d):
        to = ring4(x, d)
        i = rel * 4 + d
        return remote(cs.at[rel, to], cr.at[i], c_send.at[i], c_recv.at[i], (z, other if rel else c, to, y))

    pairs = [(rel, d) for d in (2, 1, 3, 0) for rel in (0, 1) if rel or d]
    for rel, d in pairs:
        go(c_copy(rel, d))
    for load in small[4:]:
        load.wait()
    total = res_ref[y, pl.ds(pl.multiple_of(32 * x, 32), 32), :].astype(F32)
    summed = cs[0, x]
    for rel, d in reversed(pairs):
        c_copy(rel, d).wait_recv()
        summed = summed + cr[rel * 4 + d]
    p1 = x * other + y * c
    p2 = x * c + y * other
    g_own[p2, p1, 0] = (total + summed).astype(BF16)

    def d1(o):
        return remote(g_own.at[p2, p1, 0], g_own.at[p2, p1, o], d1_send.at[o], d1_recv.at[o], (at_z(-NEAR[o]), c, x, y))

    for o in reversed(range(1, NZ)):
        go(d1(o))

    def along_first(d):
        return (z, c, ring4(x, d * other), ring4(y, d * c))

    def along_second(d):
        return (z, c, ring4(x, d * c), ring4(y, d * other))

    def d2(s, d):
        part = pl.ds(s * CHUNK, CHUNK)
        i = s * 3 + d - 1
        return remote(g_own.at[p2, p1, part], g_own.at[p2, p1, part], d2_send.at[i], d2_recv.at[i], along_first(d))

    def d2_arrival(s, d):
        part = pl.ds(s * CHUNK, CHUNK)
        i = s * 3 + d - 1
        slab = g_own.at[p2, ring4(p1, 4 - d), part]
        remote(slab, slab, d2_send.at[i], d2_recv.at[i], along_first(d)).wait_recv()

    def d3(s, e, d):
        part = pl.ds(s * CHUNK, CHUNK)
        i = (s * 4 + e) * 3 + d - 1
        slab = g_own.at[p2, ring4(p1, 4 - e), part]
        return remote(slab, slab, d3_send.at[i], d3_recv.at[i], along_second(d))

    def d3_arrival(s, e, d):
        part = pl.ds(s * CHUNK, CHUNK)
        i = (s * 4 + e) * 3 + d - 1
        slab = g_own.at[ring4(p2, 4 - d), ring4(p1, 4 - e), part]
        remote(slab, slab, d3_send.at[i], d3_recv.at[i], along_second(d)).wait_recv()

    for s in range(CHUNKS):
        for o in range(max(1, s * CHUNK), (s + 1) * CHUNK):
            d1(o).wait_recv()
        for d in (2, 1, 3):
            go(d2(s, d))
        for d in (2, 1, 3):
            go(d3(s, 0, d))
    for s in range(CHUNKS):
        for e in (1, 3, 2):
            d2_arrival(s, e)
            for d in (2, 1, 3):
                go(d3(s, e, d))
    for s in range(CHUNKS):
        for e in (0, 1, 3, 2):
            for d in (1, 3, 2):
                d3_arrival(s, e, d)

    def held(core_rows, parity, n):
        xx, yy = n % 4, 2 * core_rows + n // 4
        return xx * parity + yy * (1 - parity), xx * (1 - parity) + yy * parity

    def d4(n):
        i, j = held(other, c, n)
        return remote(g_own.at[i, j], g_other.at[i, j], d4_send.at[n], d4_recv.at[n], (z, other, x, y))

    for n in range(8):
        go(d4(n))

    def squares(ref, i, j):
        part = ref[i, j].astype(F32)
        return jnp.sum(part * part, 0)

    for n in range(8):
        i, j = held(c, c, n)
        rb[n] = squares(g_own, i, j)
    for n in range(8):
        i, j = held(c, other, n)
        remote(g_other.at[i, j], g_other.at[i, j], d4_send.at[n], d4_recv.at[n], (z, other, x, y)).wait_recv()
        total_sq = jnp.sum(rb[n] + squares(g_other, i, j), -1, keepdims=True)
        rb[n] = jnp.broadcast_to(lax.rsqrt(total_sq * (1.0 / 4096) + 1e-05), (32, 128))

    loads[3].wait()
    lm_copy_in = remote(lm_hbm, lm_buf.at[other], b_send.at[1], b_recv.at[1], (z, other, x, y))
    lm_copy_in.wait_recv()
    for o in range(NZ):
        for ref, parity in ((g_own, c), (g_other, other)):
            at = pl.multiple_of((at_z(NEAR[o]) * 2 + parity) * 128, 128)
            gain = gain_ref[:, pl.ds(at, 128)]
            for n in range(8):
                i, j = held(c, parity, n)
                normed[n * 32 : (n + 1) * 32, pl.ds(at, 128)] = (ref[i, j, o].astype(F32) * rb[n] * gain).astype(BF16)

    for half in range(2):
        acc[half] = nt_dot(lm_buf[half, :, :512], normed[:, :512])

    @pl.loop(1, 8)
    def _(t):
        lanes = pl.ds(pl.multiple_of(t * 512, 512), 512)
        for half in range(2):
            acc[half] += nt_dot(lm_buf[half, :, lanes], normed[:, lanes])

    logits = [acc[0], acc[1]]
    peak = jnp.maximum(jnp.max(logits[0], 0, keepdims=True), jnp.max(logits[1], 0, keepdims=True))
    wanted = jnp.concatenate([tgt_ref[pl.ds(2 * c, 1), :], tgt_ref[pl.ds(2 * c + 1, 1), :]], 1)
    spread = jnp.zeros((1, 256), F32)
    picked = jnp.zeros((1, 256), F32)
    for half in range(2):
        base = (((2 * z + half) * NX + x) * NY + y) * 256
        entry = base + lax.broadcasted_iota(jnp.int32, (256, 256), 0)
        spread += jnp.sum(jnp.exp(logits[half] - peak), 0, keepdims=True)
        picked += jnp.sum(jnp.where(entry == wanted, logits[half], 0.0), 0, keepdims=True)
    partial = peak + jnp.log(spread)
    for n in range(2):
        st[n, 0:1] = partial[:, n * 128 : (n + 1) * 128]
        st[n, 1:2] = picked[:, n * 128 : (n + 1) * 128]

    active = c == y // 2

    def f1(n, d, e):
        i = d * 4 + e
        return remote(st.at[n], fr.at[x * 4 + y], f1_send.at[n * 4 + d], f1_recv.at[i], (z, c, ring4(x, d), 2 * c + n))

    for n in range(2):
        e = lax.rem(2 * c + n - y + 4, 4)
        for d in (2, 1, 3):
            f1(n, d, e).start()

        @pl.when(e != 0)
        def _():
            f1(n, 0, e).start()

        @pl.when(e == 0)
        def _():
            fr[x * 4 + y] = st[n]

    def joined(ref):
        heads = [ref[n] for n in range(16)]
        high = functools.reduce(jnp.maximum, [part[0:1] for part in heads])
        mass = functools.reduce(jnp.add, [jnp.exp(part[0:1] - high) for part in heads])
        return high + jnp.log(mass), functools.reduce(jnp.add, [part[1:2] for part in heads])

    def f2(o, core, n):
        return remote(fs, zr.at[o], f2_send.at[2 * o + n], f2_recv.at[o], (at_z(-NEAR[o]), core, x, y))

    @pl.when(active)
    def _():
        for d in range(4):
            for e in range(4):
                if d or e:
                    here = fr.at[lax.rem(x + 4 - d, 4) * 4 + lax.rem(y + 4 - e, 4)]
                    remote(st.at[0], here, f1_send.at[0], f1_recv.at[d * 4 + e], (z, c, x, y)).wait_recv()
        level, hit = joined(fr)
        fs[0:1] = level
        fs[1:2] = hit
        for o in reversed(range(1, NZ)):
            f2(o, c, 0).start()
            f2(o, other, 1).start()
        f2(0, other, 1).start()
        zr[0] = fs[...]

    for o in range(1, NZ):
        f2(o, c, 0).wait_recv()

    @pl.when(jnp.logical_not(active))
    def _():
        f2(0, other, 1).wait_recv()

    level, hit = joined(zr)
    logprob = hit - level
    spots = lax.broadcasted_iota(jnp.int32, (1, 128), 1) * 64 + 31
    count = jnp.zeros((1, 1), F32)
    for n in range(4):
        count += jnp.sum(jnp.where(spots < len_ref[n], 1.0, 0.0), -1, keepdims=True)
    mine = jnp.where(spots < len_ref[y], 1.0, 0.0)
    score = jnp.sum(mine * logprob, -1, keepdims=True) / count
    out_ref[0:1] = logprob
    out_ref[1:2] = jnp.broadcast_to(score, (1, 128))

    for copy in sent:
        copy.wait_send()
    for n in range(2):
        e = lax.rem(2 * c + n - y + 4, 4)
        for d in (2, 1, 3):
            f1(n, d, e).wait_send()

        @pl.when(e != 0)
        def _():
            f1(n, 0, e).wait_send()

    @pl.when(active)
    def _():
        for o in reversed(range(1, NZ)):
            f2(o, c, 0).wait_send()
            f2(o, other, 1).wait_send()
        f2(0, other, 1).wait_send()


def body(
    queries, keys, values, key_position, compress_keys, compress_values,
    out_proj, residual, norm_gain, lm_head, targets, lengths,
):
    vmem = pl.BlockSpec(memory_space=pltpu.VMEM)
    hbm = pl.BlockSpec(memory_space=pltpu.HBM)
    dma = pltpu.SemaphoreType.DMA
    found = pl.pallas_call(
        kernel,
        out_shape=jax.ShapeDtypeStruct((2, 128), F32),
        in_specs=[hbm] * 12,
        out_specs=vmem,
        scratch_shapes=[
            pltpu.VMEM((1, 4, 1024), BF16),
            pltpu.VMEM((1, 256, 256), BF16),
            pltpu.VMEM((1, 256, 256), BF16),
            pltpu.VMEM((32, 128), F32),
            pltpu.VMEM((4, 128, 128), BF16),
            pltpu.VMEM((1, 4096), F32),
            pltpu.VMEM((4, 128), jnp.int32),
            pltpu.SMEM((4,), jnp.int32),
            pltpu.VMEM((2, 4096, 128), BF16),
            pltpu.VMEM((512, 128), BF16),
            pltpu.VMEM((512, 128), BF16),
            pltpu.VMEM((2, 256, 4096), BF16),
            pltpu.VMEM((2, 2, 256, 128), F32),
            pltpu.VMEM((2, 32, 2048), BF16),
            pltpu.VMEM((2, 48, 2048), BF16),
            pltpu.VMEM((2, 3, 16, 128), BF16),
            pltpu.VMEM((2, 4, 128), F32),
            pltpu.VMEM((2, 1, 128), F32),
            pltpu.VMEM((16, 2, 3, 16, 128), BF16),
            pltpu.VMEM((16, 2, 4, 128), F32),
            pltpu.VMEM((512, 128), BF16),
            pltpu.VMEM((512, 128), BF16),
            pltpu.VMEM((512, 128), BF16),
            pltpu.VMEM((128, 512), BF16),
            pltpu.VMEM((2, 4, 32, 128), F32),
            pltpu.VMEM((8, 32, 128), F32),
            pltpu.VMEM((4, 4, 16, 32, 128), BF16),
            pltpu.VMEM((4, 4, 16, 32, 128), BF16),
            pltpu.VMEM((8, 32, 128), F32),
            pltpu.VMEM((256, 4096), BF16),
            pltpu.VMEM((2, 256, 256), F32),
            pltpu.VMEM((2, 2, 128), F32),
            pltpu.VMEM((16, 2, 128), F32),
            pltpu.VMEM((2, 128), F32),
            pltpu.VMEM((16, 2, 128), F32),
            dma((4,)), dma((8,)),
            dma((2,)), dma((2,)),
            dma((14,)), dma((16,)),
            dma((8,)), dma((8,)),
            dma((8,)), dma((8,)),
            dma((16,)), dma((16,)),
            dma((12,)), dma((12,)),
            dma((48,)), dma((48,)),
            dma((8,)), dma((8,)),
            dma((8,)), dma((16,)),
            dma((32,)), dma((16,)),
        ],
        compiler_params=pltpu.CompilerParams(
            collective_id=0, has_side_effects=True, vmem_limit_bytes=67043328
        ),
    )(
        queries, keys, values, key_position, compress_keys, compress_values,
        out_proj, residual, norm_gain.reshape(1, -1), lm_head, targets, lengths,
    )
    seq_pos = lax.axis_index(SEQ)
    token_logprob = lax.dynamic_slice(found, (0, seq_pos * 4), (1, 4))
    return token_logprob, found[1, :1]


def solution(mesh):
    split = Mesh(
        mesh.devices.reshape(16, 2, mesh.shape["mp"], mesh.shape["batch"]),
        ("seq_0", "seq_1", "mp", "batch"),
    )
    in_specs = (
        P("batch", SEQ, "mp"),
        P("batch", SEQ, "mp"),
        P("batch", SEQ, "mp"),
        P(),
        P(),
        P(),
        P("mp", SEQ),
        P(None, None, SEQ),
        P(),
        P(SEQ_MP_BATCH, None),
        P(),
        P(),
    )
    out_specs = (P("batch", SEQ), P("batch"))
    return jax.shard_map(body, mesh=split, in_specs=in_specs, out_specs=out_specs, check_vma=False)
```

```python
import functools
import math

import jax
import jax.numpy as jnp
from jax import lax
from jax.experimental import pallas as pl
from jax.experimental.pallas import tpu as pltpu
from jax.sharding import Mesh
from jax.sharding import PartitionSpec as P

BF16 = jnp.bfloat16
F32 = jnp.float32
HEAD_DIM = 128
MESH = pl.DeviceIdType.MESH
AXES = ("seq_0", "seq_1", "mp", "batch")
SEQ = ("seq_0", "seq_1")
SEQ_MP_BATCH = ("seq_0", "seq_1", "mp", "batch")
NZ, NX, NY = 16, 4, 4

SHIFT = (0, 1, 2, -1, -2)
STEP = (0, 5, -5)
OFFSETS = tuple(s + w for s in SHIFT for w in STEP) + (8,)
ROUND_ONE = (1, 2, 6, 12, 3, 9, 0)
SLOT_OF = {off % NZ: k for k, off in enumerate(OFFSETS)}
NEAR = (0, 1, -1, 2, -2, 3, -3, 4, -4, 5, -5, 6, -6, 7, -7, 8)
CHUNK = 4
CHUNKS = NZ // CHUNK
LAST = CHUNKS - 1


def nt_dot(a, b):
    return lax.dot_general(a, b, (((1,), (1,)), ((), ())), preferred_element_type=F32)


def kernel(
    q_hbm, k_hbm, v_hbm, pos_hbm, wk_hbm, wv_hbm, op_hbm, res_hbm, gain_hbm, lm_hbm, tgt_hbm, len_hbm,
    out_ref,
    q_ref, k_ref, v_ref, pos_ref, res_ref, gain_ref, tgt_ref, len_ref, w_buf, op_own, op_other, lm_buf, rows_f, xa, xb, pay, epay, bz, kvq, ebuf, qperm, kmat, vmat, att,
    cs, cr, g_own, g_other, rb, normed, acc, st, fr, fs, zr,
    local_sem, small_sem, b_send, b_recv, a1_send, a1_recv, a2_send, a2_recv, c_send, c_recv, d1_send, d1_recv,
    d2_send, d2_recv, d3_send, d3_recv, d4_send, d4_recv, f1_send, f1_recv, f2_send, f2_recv,
):
    z, c, x, y = (lax.axis_index(name) for name in AXES)
    other = 1 - c

    def at_z(off):
        return lax.rem(z + (off + NZ), NZ)

    def ring4(p, d):
        return lax.rem(p + d, 4)

    barrier = pltpu.get_barrier_semaphore()
    peers = [(at_z(off), core, x, y) for off in range(1, NZ) for core in (0, 1)]
    peers += [(z, other, ring4(x, d), y) for d in range(4)]
    peers += [(z, c, ring4(x, d), ring4(y, e)) for d in range(4) for e in range(4) if d or e]
    for peer in peers:
        pl.semaphore_signal(barrier, inc=1, device_id=peer, device_id_type=MESH)

    loads = [
        pltpu.make_async_copy(wk_hbm, w_buf.at[0], local_sem.at[0]),
        pltpu.make_async_copy(wv_hbm, w_buf.at[1], local_sem.at[1]),
        pltpu.make_async_copy(op_hbm.at[pl.ds(pl.multiple_of(c * 512, 512), 512)], op_own, local_sem.at[2]),
        pltpu.make_async_copy(lm_hbm, lm_buf.at[c], local_sem.at[3]),
    ]
    small = [
        pltpu.make_async_copy(src, dst, small_sem.at[n])
        for n, (src, dst) in enumerate((
            (k_hbm, k_ref), (v_hbm, v_ref), (pos_hbm, pos_ref), (q_hbm, q_ref),
            (res_hbm, res_ref), (gain_hbm, gain_ref), (tgt_hbm, tgt_ref), (len_hbm, len_ref),
        ))
    ]
    for load in small[:4] + loads + small[4:]:
        load.start()
    for load in small[:4]:
        load.wait()

    for t, src in enumerate((k_ref, v_ref)):
        for h in range(2):
            rows_f[t, h] = src[0, :, h * 128 : (h + 1) * 128].astype(F32)
    for i in range(16):
        lanes = slice(i * 128, (i + 1) * 128)
        pa, pb = pos_ref[i : i + 1, :], pos_ref[16 + i : 17 + i, :]
        for t in range(2):
            for h in range(2):
                rows = rows_f[t, h, pl.ds(i, 16, stride=16), :]
                xa[t, h * 16 : (h + 1) * 16, lanes] = (rows + pa).astype(BF16)
                xb[t, h * 16 : (h + 1) * 16, lanes] = (rows + pb).astype(BF16)
            xb[t, 32:48, lanes] = jnp.broadcast_to(pb, (16, 128)).astype(BF16)
    qf = q_ref[0].astype(F32)
    for h in range(2):
        lines = [qf[:, (4 * h + g) * 128 : (4 * h + g + 1) * 128] for g in range(4)]
        pay[h, 2] = jnp.concatenate(lines, 0).astype(BF16)
    for t in range(2):
        loads[t].wait()
        first = jnp.dot(xa[t], w_buf[t, :2048], preferred_element_type=F32)
        second = jnp.dot(xb[t], w_buf[t, 2048:], preferred_element_type=F32)
        bz[t] = second[32:33]
        for h in range(2):
            fh, sh = first[h * 16 : (h + 1) * 16], second[h * 16 : (h + 1) * 16]
            pay[h, t] = (fh + pltpu.roll(sh, 15, 0)).astype(BF16)
            epay[h, 2 * t : 2 * t + 1] = fh[15:16]
            epay[h, 2 * t + 1 : 2 * t + 2] = sh[0:1]
    kvq[0, c] = pay[c]
    ebuf[0, c] = epay[c]

    pl.semaphore_wait(barrier, len(peers))

    def remote(src, dst, send, recv, peer):
        return pltpu.make_async_remote_copy(
            src_ref=src, dst_ref=dst, send_sem=send, recv_sem=recv, device_id=peer, device_id_type=MESH
        )

    sent = []

    def go(copy):
        copy.start()
        sent.append(copy)

    def a1(n, k, core, h):
        peer = (at_z(-OFFSETS[k]), core, x, y)
        i, j = 4 * ROUND_ONE.index(k) + 2 * n, 4 * ROUND_ONE.index(k) + 2 * c
        return (
            remote(pay.at[h], kvq.at[k, c], a1_send.at[i], a1_recv.at[j], peer),
            remote(epay.at[h], ebuf.at[k, c], a1_send.at[i + 1], a1_recv.at[j + 1], peer),
        )

    for k in ROUND_ONE[:-1]:
        for n, h in enumerate((c, other)):
            for part in a1(n, k, h, h):
                go(part)
    for part in a1(0, 0, other, other):
        go(part)

    op_copy = remote(op_hbm.at[pl.ds(pl.multiple_of(other * 512, 512), 512)], op_other, b_send.at[0], b_recv.at[0], (z, other, x, y))
    lm_copy = remote(lm_hbm, lm_buf.at[c], b_send.at[1], b_recv.at[1], (z, other, x, y))
    go(op_copy)
    go(lm_copy)

    def a1_arrival(k, core):
        j = 4 * ROUND_ONE.index(k) + 2 * core
        remote(pay.at[0], kvq.at[k, core], a1_send.at[0], a1_recv.at[j], (z, c, x, y)).wait_recv()
        remote(epay.at[0], ebuf.at[k, core], a1_send.at[0], a1_recv.at[j + 1], (z, c, x, y)).wait_recv()

    for k in (1, 2):
        for core in range(2):
            a1_arrival(k, core)

    def a2(g):
        peer = (at_z(-SHIFT[g]), c, x, y)
        src, dst, i = pl.ds(1, 2), pl.ds(3 * g + 1, 2), 2 * g - 2
        return (
            remote(kvq.at[src], kvq.at[dst], a2_send.at[i], a2_recv.at[i], peer),
            remote(ebuf.at[src], ebuf.at[dst], a2_send.at[i + 1], a2_recv.at[i + 1], peer),
        )

    def a2_far(n):
        peer = (at_z(-3 if n == 0 else 3), c, x, y)
        i = 8 + 2 * n
        return (
            remote(kvq.at[1 + n, n], kvq.at[15, n], a2_send.at[i], a2_recv.at[i], peer),
            remote(ebuf.at[1 + n, n], ebuf.at[15, n], a2_send.at[i + 1], a2_recv.at[i + 1], peer),
        )

    for n in (0, 1):
        for part in a2_far(n):
            go(part)
    for g in (2, 4, 1, 3):
        for part in a2(g):
            go(part)

    col = lax.broadcasted_iota(jnp.int32, (1, 512), 1)
    slot, core_of, lane = col // 32, (col // 16) % 2, col % 16
    g_of, w_of = slot // 3, slot % 3
    off_of = jnp.where(g_of > 2, 2 - g_of, g_of) + jnp.where(w_of == 2, -5, 5 * w_of)
    off_of = jnp.where(slot == 15, 8, off_of)
    seq_of = ((off_of + z + NZ) % NZ) * 2 + core_of
    block_of = seq_of * 16 + lane
    row_of = (lane // 4) * 128 + seq_of * 4 + lane % 4
    perm = jnp.where(lax.broadcasted_iota(jnp.int32, (512, 512), 0) == row_of, 1.0, 0.0).astype(BF16)

    a1_arrival(0, other)
    for k in (3, 9, 6, 12):
        for core in range(2):
            a1_arrival(k, core)
    for g in (1, 3, 2, 4):
        for part in a2(g):
            part.wait_recv()
    for n in (0, 1):
        for part in a2_far(n):
            part.wait_recv()

    q_all = kvq[:, :, 2].reshape(512, 128)
    qperm[...] = jnp.dot(perm, q_all, preferred_element_type=F32).astype(BF16)
    last = lax.broadcasted_iota(jnp.int32, (16, 128), 0) == 15
    for k in range(NZ):
        top = (at_z(OFFSETS[k]) == NZ - 1).astype(F32)
        after = SLOT_OF[(OFFSETS[k] + 1) % NZ]
        for t, mat in enumerate((kmat, vmat)):
            for core in range(2):
                if core == 0:
                    beyond = ebuf[k, 1, 2 * t + 1 : 2 * t + 2]
                else:
                    beyond = ebuf[after, 0, 2 * t + 1 : 2 * t + 2] * (1.0 - top) + bz[t] * top
                fixed = ebuf[k, core, 2 * t : 2 * t + 1] + beyond
                tile = jnp.where(last, fixed, kvq[k, core, t].astype(F32))
                mat[(2 * k + core) * 16 : (2 * k + core + 1) * 16, :] = tile.astype(BF16)

    limit = lax.broadcasted_iota(jnp.int32, (128, 1), 0) * 4
    visible = block_of <= limit
    for g in range(4):
        score = nt_dot(qperm[g * 128 : (g + 1) * 128], kmat[...]) * (1.0 / math.sqrt(HEAD_DIM))
        score = jnp.where(visible, score, -1e30)
        peak = jnp.max(score, -1, keepdims=True)
        weight = jnp.where(visible, jnp.exp(score - peak), 0.0)
        prob = (weight * (1.0 / jnp.sum(weight, -1, keepdims=True))).astype(BF16)
        found = jnp.dot(prob, vmat[...], preferred_element_type=F32)
        att[:, g * 128 : (g + 1) * 128] = found.astype(BF16)

    loads[2].wait()
    cs[0] = jnp.dot(att[...], op_own[...], preferred_element_type=F32).reshape(4, 32, 128)
    op_copy.wait_recv()
    cs[1] = jnp.dot(att[...], op_other[...], preferred_element_type=F32).reshape(4, 32, 128)

    def c_copy(rel, d):
        to = ring4(x, d)
        i = rel * 4 + d
        return remote(cs.at[rel, to], cr.at[i], c_send.at[i], c_recv.at[i], (z, other if rel else c, to, y))

    pairs = [(rel, d) for d in (2, 1, 3, 0) for rel in (0, 1) if rel or d]
    for rel, d in pairs:
        go(c_copy(rel, d))
    for load in small[4:]:
        load.wait()
    total = res_ref[y, pl.ds(pl.multiple_of(32 * x, 32), 32), :].astype(F32)
    summed = cs[0, x]
    for rel, d in reversed(pairs):
        c_copy(rel, d).wait_recv()
        summed = summed + cr[rel * 4 + d]
    p1 = x * other + y * c
    p2 = x * c + y * other
    g_own[p2, p1, 0] = (total + summed).astype(BF16)

    def d1(o):
        return remote(g_own.at[p2, p1, 0], g_own.at[p2, p1, o], d1_send.at[o], d1_recv.at[o], (at_z(-NEAR[o]), c, x, y))

    for o in reversed(range(1, NZ)):
        go(d1(o))

    def along_first(d):
        return (z, c, ring4(x, d * other), ring4(y, d * c))

    def along_second(d):
        return (z, c, ring4(x, d * c), ring4(y, d * other))

    SIDE = {1: 0, 3: 1, 2: 2}

    def whole(s):
        return pl.ds(s * CHUNK, CHUNK)

    def half(s, n):
        return pl.ds(s * CHUNK + n * (CHUNK // 2), CHUNK // 2)

    def first(slab, i, d):
        return remote(slab, slab, d2_send.at[i], d2_recv.at[i], along_first(d))

    def second(slab, i, d):
        return remote(slab, slab, d3_send.at[i], d3_recv.at[i], along_second(d))

    def slab1(e, part):
        return g_own.at[p2, ring4(p1, (4 - e) % 4), part]

    def slab2(d, e, part):
        return g_own.at[ring4(p2, (4 - d) % 4), ring4(p1, (4 - e) % 4), part]

    def send_first(s):
        for d in (2, 1, 3) if s == LAST else (1, 3):
            go(first(slab1(0, whole(s)), s * 4 + SIDE[d], d))

    def send_second(s, e):
        for d in (2, 1, 3) if s == LAST else (1, 3):
            go(second(slab1(e, whole(s)), (s * 4 + e) * 4 + SIDE[d], d))

    def on_first(s, e):
        if e == 2 and s < LAST:
            for n in range(2):
                first(slab1(2, half(s, n)), s * 4 + 2 + n, 1).wait_recv()
        else:
            first(slab1(e, whole(s)), s * 4 + SIDE[e], 1).wait_recv()
            if s < LAST:
                go(first(slab1(e, half(s, SIDE[e])), s * 4 + 2 + SIDE[e], e))
        send_second(s, e)

    def on_second(s, e, d):
        base = (s * 4 + e) * 4
        if d == 2 and s < LAST:
            for n in range(2):
                second(slab2(2, e, half(s, n)), base + 2 + n, 1).wait_recv()
        else:
            second(slab2(d, e, whole(s)), base + SIDE[d], 1).wait_recv()
            if s < LAST:
                go(second(slab2(d, e, half(s, SIDE[d])), base + 2 + SIDE[d], d))

    def on_origin(s):
        for o in range(max(1, s * CHUNK), (s + 1) * CHUNK):
            d1(o).wait_recv()
        send_first(s)
        send_second(s, 0)

    def held(core_rows, parity, n):
        xx, yy = n % 4, 2 * core_rows + n // 4
        return xx * parity + yy * (1 - parity), xx * (1 - parity) + yy * parity

    def d4(s, n, rows, parity, src, dst):
        i, j = held(rows, parity, n)
        k = s * 8 + n
        return remote(src.at[i, j, whole(s)], dst.at[i, j, whole(s)], d4_send.at[k], d4_recv.at[k], (z, other, x, y))

    def squares(ref, s, rows, parity, n):
        i, j = held(rows, parity, n)
        part = ref[i, j, s * CHUNK : (s + 1) * CHUNK].astype(F32)
        return jnp.sum(part * part, 0)

    def on_complete(s):
        for n in range(8):
            go(d4(s, n, other, c, g_own, g_other))
        for n in range(8):
            found = squares(g_own, s, c, c, n)
            rb[n] = found if s == 0 else rb[n] + found

    events = []
    for s in range(CHUNKS):
        start = 3.0 + 2.0 * s
        twice = 3.5 if s == LAST else 5.6
        events.append((start, s, 0, functools.partial(on_origin, s)))
        latest = start
        for e in (0, 1, 3, 2):
            ready = start + (0.0, 2.8, twice, 2.8)[e]
            if e:
                events.append((ready, s, 1, functools.partial(on_first, s, e)))
            for d in (1, 3, 2):
                arrival = ready + (0.0, 2.8, twice, 2.8)[d]
                latest = max(latest, arrival)
                events.append((arrival, s, 2, functools.partial(on_second, s, e, d)))
        events.append((latest, s, 3, functools.partial(on_complete, s)))
    for event in sorted(events, key=lambda item: item[:3]):
        event[3]()

    for s in range(CHUNKS):
        for n in range(8):
            d4(s, n, c, other, g_other, g_other).wait_recv()
            rb[n] = rb[n] + squares(g_other, s, c, other, n)
    for n in range(8):
        total_sq = jnp.sum(rb[n], -1, keepdims=True)
        rb[n] = jnp.broadcast_to(lax.rsqrt(total_sq * (1.0 / 4096) + 1e-05), (32, 128))

    loads[3].wait()
    lm_copy_in = remote(lm_hbm, lm_buf.at[other], b_send.at[1], b_recv.at[1], (z, other, x, y))
    lm_copy_in.wait_recv()
    for o in range(NZ):
        for ref, parity in ((g_own, c), (g_other, other)):
            at = pl.multiple_of((at_z(NEAR[o]) * 2 + parity) * 128, 128)
            gain = gain_ref[:, pl.ds(at, 128)]
            for n in range(8):
                i, j = held(c, parity, n)
                tile = (ref[i, j, o].astype(F32) * rb[n] * gain).astype(BF16)
                normed[o, n * 32 : (n + 1) * 32, pl.ds(pl.multiple_of(parity * 128, 128), 128)] = tile
        if o % 2:
            for part in range(2):
                grown = 0.0 if o == 1 else acc[part]
                for k in (o - 1, o):
                    lanes = pl.ds(pl.multiple_of(at_z(NEAR[k]) * 256, 256), 256)
                    grown = grown + nt_dot(lm_buf[part, :, lanes], normed[k])
                acc[part] = grown

    logits = [acc[0], acc[1]]
    peak = jnp.maximum(jnp.max(logits[0], 0, keepdims=True), jnp.max(logits[1], 0, keepdims=True))
    wanted = jnp.concatenate([tgt_ref[pl.ds(2 * c, 1), :], tgt_ref[pl.ds(2 * c + 1, 1), :]], 1)
    spread = jnp.zeros((1, 256), F32)
    picked = jnp.zeros((1, 256), F32)
    for half in range(2):
        base = (((2 * z + half) * NX + x) * NY + y) * 256
        entry = base + lax.broadcasted_iota(jnp.int32, (256, 256), 0)
        spread += jnp.sum(jnp.exp(logits[half] - peak), 0, keepdims=True)
        picked += jnp.sum(jnp.where(entry == wanted, logits[half], 0.0), 0, keepdims=True)
    partial = peak + jnp.log(spread)
    for n in range(2):
        st[n, 0:1] = partial[:, n * 128 : (n + 1) * 128]
        st[n, 1:2] = picked[:, n * 128 : (n + 1) * 128]

    active = c == y // 2

    def f1(n, d, e):
        i = d * 4 + e
        return remote(st.at[n], fr.at[x * 4 + y], f1_send.at[n * 4 + d], f1_recv.at[i], (z, c, ring4(x, d), 2 * c + n))

    for n in range(2):
        e = lax.rem(2 * c + n - y + 4, 4)
        for d in (2, 1, 3):
            f1(n, d, e).start()

        @pl.when(e != 0)
        def _():
            f1(n, 0, e).start()

        @pl.when(e == 0)
        def _():
            fr[x * 4 + y] = st[n]

    def joined(ref):
        heads = [ref[n] for n in range(16)]
        high = functools.reduce(jnp.maximum, [part[0:1] for part in heads])
        mass = functools.reduce(jnp.add, [jnp.exp(part[0:1] - high) for part in heads])
        return high + jnp.log(mass), functools.reduce(jnp.add, [part[1:2] for part in heads])

    def f2(o, core, n):
        return remote(fs, zr.at[o], f2_send.at[2 * o + n], f2_recv.at[o], (at_z(-NEAR[o]), core, x, y))

    @pl.when(active)
    def _():
        for d in range(4):
            for e in range(4):
                if d or e:
                    here = fr.at[lax.rem(x + 4 - d, 4) * 4 + lax.rem(y + 4 - e, 4)]
                    remote(st.at[0], here, f1_send.at[0], f1_recv.at[d * 4 + e], (z, c, x, y)).wait_recv()
        level, hit = joined(fr)
        fs[0:1] = level
        fs[1:2] = hit
        for o in reversed(range(1, NZ)):
            f2(o, c, 0).start()
            f2(o, other, 1).start()
        f2(0, other, 1).start()
        zr[0] = fs[...]

    for o in range(1, NZ):
        f2(o, c, 0).wait_recv()

    @pl.when(jnp.logical_not(active))
    def _():
        f2(0, other, 1).wait_recv()

    level, hit = joined(zr)
    logprob = hit - level
    spots = lax.broadcasted_iota(jnp.int32, (1, 128), 1) * 64 + 31
    count = jnp.zeros((1, 1), F32)
    for n in range(4):
        count += jnp.sum(jnp.where(spots < len_ref[n], 1.0, 0.0), -1, keepdims=True)
    mine = jnp.where(spots < len_ref[y], 1.0, 0.0)
    score = jnp.sum(mine * logprob, -1, keepdims=True) / count
    out_ref[0:1] = logprob
    out_ref[1:2] = jnp.broadcast_to(score, (1, 128))

    for copy in sent:
        copy.wait_send()
    for n in range(2):
        e = lax.rem(2 * c + n - y + 4, 4)
        for d in (2, 1, 3):
            f1(n, d, e).wait_send()

        @pl.when(e != 0)
        def _():
            f1(n, 0, e).wait_send()

    @pl.when(active)
    def _():
        for o in reversed(range(1, NZ)):
            f2(o, c, 0).wait_send()
            f2(o, other, 1).wait_send()
        f2(0, other, 1).wait_send()


def body(
    queries, keys, values, key_position, compress_keys, compress_values,
    out_proj, residual, norm_gain, lm_head, targets, lengths,
):
    vmem = pl.BlockSpec(memory_space=pltpu.VMEM)
    hbm = pl.BlockSpec(memory_space=pltpu.HBM)
    dma = pltpu.SemaphoreType.DMA
    found = pl.pallas_call(
        kernel,
        out_shape=jax.ShapeDtypeStruct((2, 128), F32),
        in_specs=[hbm] * 12,
        out_specs=vmem,
        scratch_shapes=[
            pltpu.VMEM((1, 4, 1024), BF16),
            pltpu.VMEM((1, 256, 256), BF16),
            pltpu.VMEM((1, 256, 256), BF16),
            pltpu.VMEM((32, 128), F32),
            pltpu.VMEM((4, 128, 128), BF16),
            pltpu.VMEM((1, 4096), F32),
            pltpu.VMEM((4, 128), jnp.int32),
            pltpu.SMEM((4,), jnp.int32),
            pltpu.VMEM((2, 4096, 128), BF16),
            pltpu.VMEM((512, 128), BF16),
            pltpu.VMEM((512, 128), BF16),
            pltpu.VMEM((2, 256, 4096), BF16),
            pltpu.VMEM((2, 2, 256, 128), F32),
            pltpu.VMEM((2, 32, 2048), BF16),
            pltpu.VMEM((2, 48, 2048), BF16),
            pltpu.VMEM((2, 3, 16, 128), BF16),
            pltpu.VMEM((2, 4, 128), F32),
            pltpu.VMEM((2, 1, 128), F32),
            pltpu.VMEM((16, 2, 3, 16, 128), BF16),
            pltpu.VMEM((16, 2, 4, 128), F32),
            pltpu.VMEM((512, 128), BF16),
            pltpu.VMEM((512, 128), BF16),
            pltpu.VMEM((512, 128), BF16),
            pltpu.VMEM((128, 512), BF16),
            pltpu.VMEM((2, 4, 32, 128), F32),
            pltpu.VMEM((8, 32, 128), F32),
            pltpu.VMEM((4, 4, 16, 32, 128), BF16),
            pltpu.VMEM((4, 4, 16, 32, 128), BF16),
            pltpu.VMEM((8, 32, 128), F32),
            pltpu.VMEM((16, 256, 256), BF16),
            pltpu.VMEM((2, 256, 256), F32),
            pltpu.VMEM((2, 2, 128), F32),
            pltpu.VMEM((16, 2, 128), F32),
            pltpu.VMEM((2, 128), F32),
            pltpu.VMEM((16, 2, 128), F32),
            dma((4,)), dma((8,)),
            dma((2,)), dma((2,)),
            dma((28,)), dma((28,)),
            dma((12,)), dma((12,)),
            dma((8,)), dma((8,)),
            dma((16,)), dma((16,)),
            dma((16,)), dma((16,)),
            dma((64,)), dma((64,)),
            dma((32,)), dma((32,)),
            dma((8,)), dma((16,)),
            dma((32,)), dma((16,)),
        ],
        compiler_params=pltpu.CompilerParams(
            collective_id=0, has_side_effects=True, vmem_limit_bytes=67043328
        ),
    )(
        queries, keys, values, key_position, compress_keys, compress_values,
        out_proj, residual, norm_gain.reshape(1, -1), lm_head, targets, lengths,
    )
    seq_pos = lax.axis_index(SEQ)
    token_logprob = lax.dynamic_slice(found, (0, seq_pos * 4), (1, 4))
    return token_logprob, found[1, :1]


def solution(mesh):
    split = Mesh(
        mesh.devices.reshape(16, 2, mesh.shape["mp"], mesh.shape["batch"]),
        ("seq_0", "seq_1", "mp", "batch"),
    )
    in_specs = (
        P("batch", SEQ, "mp"),
        P("batch", SEQ, "mp"),
        P("batch", SEQ, "mp"),
        P(),
        P(),
        P(),
        P("mp", SEQ),
        P(None, None, SEQ),
        P(),
        P(SEQ_MP_BATCH, None),
        P(),
        P(),
    )
    out_specs = (P("batch", SEQ), P("batch"))
    return jax.shard_map(body, mesh=split, in_specs=in_specs, out_specs=out_specs, check_vma=False)
```

```python
import functools
import math

import jax
import jax.numpy as jnp
from jax import lax
from jax.experimental import pallas as pl
from jax.experimental.pallas import tpu as pltpu
from jax.sharding import Mesh
from jax.sharding import PartitionSpec as P

BF16 = jnp.bfloat16
F32 = jnp.float32
HEAD_DIM = 128
MESH = pl.DeviceIdType.MESH
AXES = ("seq_0", "seq_1", "mp", "batch")
SEQ = ("seq_0", "seq_1")
SEQ_MP_BATCH = ("seq_0", "seq_1", "mp", "batch")
NZ, NX, NY = 16, 4, 4

SHIFT = (0, 1, 2, -1, -2)
STEP = (0, 5, -5)
OFFSETS = tuple(s + w for s in SHIFT for w in STEP) + (8,)
ROUND_ONE = (1, 2, 6, 12, 3, 9, 0)
SLOT_OF = {off % NZ: k for k, off in enumerate(OFFSETS)}
NEAR = (0, 1, -1, 2, -2, 3, -3, 4, -4, 5, -5, 6, -6, 7, -7, 8)
CHUNK = 4
MODE = 0
ORDER = (1, 3, 2)
CHUNKS = NZ // CHUNK
LAST = CHUNKS - 1


def nt_dot(a, b):
    return lax.dot_general(a, b, (((1,), (1,)), ((), ())), preferred_element_type=F32)


def kernel(
    q_hbm, k_hbm, v_hbm, pos_hbm, wk_hbm, wv_hbm, op_hbm, res_hbm, gain_hbm, lm_hbm, tgt_hbm, len_hbm,
    out_ref,
    q_ref, k_ref, v_ref, pos_ref, res_ref, gain_ref, tgt_ref, len_ref, w_buf, op_own, op_other, lm_buf, rows_f, xa, xb, pay, epay, bz, kvq, ebuf, qperm, kmat, vmat, att,
    cs, cr, g_own, g_other, rb, normed, acc, st, fr, fs, zr,
    local_sem, small_sem, b_send, b_recv, a1_send, a1_recv, a2_send, a2_recv, c_send, c_recv, d1_send, d1_recv,
    d2_send, d2_recv, d3_send, d3_recv, d4_send, d4_recv, f1_send, f1_recv, f2_send, f2_recv,
):
    z, c, x, y = (lax.axis_index(name) for name in AXES)
    other = 1 - c

    def at_z(off):
        return lax.rem(z + (off + NZ), NZ)

    def ring4(p, d):
        return lax.rem(p + d, 4)

    barrier = pltpu.get_barrier_semaphore()
    peers = [(at_z(off), core, x, y) for off in range(1, NZ) for core in (0, 1)]
    peers += [(z, other, ring4(x, d), y) for d in range(4)]
    peers += [(z, c, ring4(x, d), ring4(y, e)) for d in range(4) for e in range(4) if d or e]
    for peer in peers:
        pl.semaphore_signal(barrier, inc=1, device_id=peer, device_id_type=MESH)

    loads = [
        pltpu.make_async_copy(wk_hbm, w_buf.at[0], local_sem.at[0]),
        pltpu.make_async_copy(wv_hbm, w_buf.at[1], local_sem.at[1]),
        pltpu.make_async_copy(op_hbm.at[pl.ds(pl.multiple_of(c * 512, 512), 512)], op_own, local_sem.at[2]),
        pltpu.make_async_copy(lm_hbm, lm_buf.at[c], local_sem.at[3]),
    ]
    small = [
        pltpu.make_async_copy(src, dst, small_sem.at[n])
        for n, (src, dst) in enumerate((
            (k_hbm, k_ref), (v_hbm, v_ref), (pos_hbm, pos_ref), (q_hbm, q_ref),
            (res_hbm, res_ref), (gain_hbm, gain_ref), (tgt_hbm, tgt_ref), (len_hbm, len_ref),
        ))
    ]
    for load in small[:4] + loads + small[4:]:
        load.start()
    for load in small[:4]:
        load.wait()

    for t, src in enumerate((k_ref, v_ref)):
        for h in range(2):
            rows_f[t, h] = src[0, :, h * 128 : (h + 1) * 128].astype(F32)
    for i in range(16):
        lanes = slice(i * 128, (i + 1) * 128)
        pa, pb = pos_ref[i : i + 1, :], pos_ref[16 + i : 17 + i, :]
        for t in range(2):
            for h in range(2):
                rows = rows_f[t, h, pl.ds(i, 16, stride=16), :]
                xa[t, h * 16 : (h + 1) * 16, lanes] = (rows + pa).astype(BF16)
                xb[t, h * 16 : (h + 1) * 16, lanes] = (rows + pb).astype(BF16)
            xb[t, 32:48, lanes] = jnp.broadcast_to(pb, (16, 128)).astype(BF16)
    qf = q_ref[0].astype(F32)
    for h in range(2):
        lines = [qf[:, (4 * h + g) * 128 : (4 * h + g + 1) * 128] for g in range(4)]
        pay[h, 2] = jnp.concatenate(lines, 0).astype(BF16)
    for t in range(2):
        loads[t].wait()
        first = jnp.dot(xa[t], w_buf[t, :2048], preferred_element_type=F32)
        second = jnp.dot(xb[t], w_buf[t, 2048:], preferred_element_type=F32)
        bz[t] = second[32:33]
        for h in range(2):
            fh, sh = first[h * 16 : (h + 1) * 16], second[h * 16 : (h + 1) * 16]
            pay[h, t] = (fh + pltpu.roll(sh, 15, 0)).astype(BF16)
            epay[h, 2 * t : 2 * t + 1] = fh[15:16]
            epay[h, 2 * t + 1 : 2 * t + 2] = sh[0:1]
    kvq[0, c] = pay[c]
    ebuf[0, c] = epay[c]

    pl.semaphore_wait(barrier, len(peers))

    def remote(src, dst, send, recv, peer):
        return pltpu.make_async_remote_copy(
            src_ref=src, dst_ref=dst, send_sem=send, recv_sem=recv, device_id=peer, device_id_type=MESH
        )

    sent = []

    def go(copy):
        copy.start()
        sent.append(copy)

    def a1(n, k, core, h):
        peer = (at_z(-OFFSETS[k]), core, x, y)
        i, j = 4 * ROUND_ONE.index(k) + 2 * n, 4 * ROUND_ONE.index(k) + 2 * c
        return (
            remote(pay.at[h], kvq.at[k, c], a1_send.at[i], a1_recv.at[j], peer),
            remote(epay.at[h], ebuf.at[k, c], a1_send.at[i + 1], a1_recv.at[j + 1], peer),
        )

    for k in ROUND_ONE[:-1]:
        for n, h in enumerate((c, other)):
            for part in a1(n, k, h, h):
                go(part)
    for part in a1(0, 0, other, other):
        go(part)

    op_copy = remote(op_hbm.at[pl.ds(pl.multiple_of(other * 512, 512), 512)], op_other, b_send.at[0], b_recv.at[0], (z, other, x, y))
    lm_copy = remote(lm_hbm, lm_buf.at[c], b_send.at[1], b_recv.at[1], (z, other, x, y))
    go(op_copy)
    go(lm_copy)

    def a1_arrival(k, core):
        j = 4 * ROUND_ONE.index(k) + 2 * core
        remote(pay.at[0], kvq.at[k, core], a1_send.at[0], a1_recv.at[j], (z, c, x, y)).wait_recv()
        remote(epay.at[0], ebuf.at[k, core], a1_send.at[0], a1_recv.at[j + 1], (z, c, x, y)).wait_recv()

    for k in (1, 2):
        for core in range(2):
            a1_arrival(k, core)

    def a2(g):
        peer = (at_z(-SHIFT[g]), c, x, y)
        src, dst, i = pl.ds(1, 2), pl.ds(3 * g + 1, 2), 2 * g - 2
        return (
            remote(kvq.at[src], kvq.at[dst], a2_send.at[i], a2_recv.at[i], peer),
            remote(ebuf.at[src], ebuf.at[dst], a2_send.at[i + 1], a2_recv.at[i + 1], peer),
        )

    def a2_far(n):
        peer = (at_z(-3 if n == 0 else 3), c, x, y)
        i = 8 + 2 * n
        return (
            remote(kvq.at[1 + n, n], kvq.at[15, n], a2_send.at[i], a2_recv.at[i], peer),
            remote(ebuf.at[1 + n, n], ebuf.at[15, n], a2_send.at[i + 1], a2_recv.at[i + 1], peer),
        )

    for n in (0, 1):
        for part in a2_far(n):
            go(part)
    for g in (2, 4, 1, 3):
        for part in a2(g):
            go(part)

    col = lax.broadcasted_iota(jnp.int32, (1, 512), 1)
    slot, core_of, lane = col // 32, (col // 16) % 2, col % 16
    g_of, w_of = slot // 3, slot % 3
    off_of = jnp.where(g_of > 2, 2 - g_of, g_of) + jnp.where(w_of == 2, -5, 5 * w_of)
    off_of = jnp.where(slot == 15, 8, off_of)
    seq_of = ((off_of + z + NZ) % NZ) * 2 + core_of
    block_of = seq_of * 16 + lane
    row_of = (lane // 4) * 128 + seq_of * 4 + lane % 4
    perm = jnp.where(lax.broadcasted_iota(jnp.int32, (512, 512), 0) == row_of, 1.0, 0.0).astype(BF16)

    a1_arrival(0, other)
    for k in (3, 9, 6, 12):
        for core in range(2):
            a1_arrival(k, core)
    for g in (1, 3, 2, 4):
        for part in a2(g):
            part.wait_recv()
    for n in (0, 1):
        for part in a2_far(n):
            part.wait_recv()

    q_all = kvq[:, :, 2].reshape(512, 128)
    qperm[...] = jnp.dot(perm, q_all, preferred_element_type=F32).astype(BF16)
    last = lax.broadcasted_iota(jnp.int32, (16, 128), 0) == 15
    for k in range(NZ):
        top = (at_z(OFFSETS[k]) == NZ - 1).astype(F32)
        after = SLOT_OF[(OFFSETS[k] + 1) % NZ]
        for t, mat in enumerate((kmat, vmat)):
            for core in range(2):
                if core == 0:
                    beyond = ebuf[k, 1, 2 * t + 1 : 2 * t + 2]
                else:
                    beyond = ebuf[after, 0, 2 * t + 1 : 2 * t + 2] * (1.0 - top) + bz[t] * top
                fixed = ebuf[k, core, 2 * t : 2 * t + 1] + beyond
                tile = jnp.where(last, fixed, kvq[k, core, t].astype(F32))
                mat[(2 * k + core) * 16 : (2 * k + core + 1) * 16, :] = tile.astype(BF16)

    limit = lax.broadcasted_iota(jnp.int32, (128, 1), 0) * 4
    visible = block_of <= limit
    for g in range(4):
        score = nt_dot(qperm[g * 128 : (g + 1) * 128], kmat[...]) * (1.0 / math.sqrt(HEAD_DIM))
        score = jnp.where(visible, score, -1e30)
        peak = jnp.max(score, -1, keepdims=True)
        weight = jnp.where(visible, jnp.exp(score - peak), 0.0)
        prob = (weight * (1.0 / jnp.sum(weight, -1, keepdims=True))).astype(BF16)
        found = jnp.dot(prob, vmat[...], preferred_element_type=F32)
        att[:, g * 128 : (g + 1) * 128] = found.astype(BF16)

    loads[2].wait()
    cs[0] = jnp.dot(att[...], op_own[...], preferred_element_type=F32).reshape(4, 32, 128)
    op_copy.wait_recv()
    cs[1] = jnp.dot(att[...], op_other[...], preferred_element_type=F32).reshape(4, 32, 128)

    def c_copy(rel, d):
        to = ring4(x, d)
        i = rel * 4 + d
        return remote(cs.at[rel, to], cr.at[i], c_send.at[i], c_recv.at[i], (z, other if rel else c, to, y))

    pairs = [(rel, d) for d in (2, 1, 3, 0) for rel in (0, 1) if rel or d]
    for rel, d in pairs:
        go(c_copy(rel, d))
    for load in small[4:]:
        load.wait()
    total = res_ref[y, pl.ds(pl.multiple_of(32 * x, 32), 32), :].astype(F32)
    summed = cs[0, x]
    for rel, d in reversed(pairs):
        c_copy(rel, d).wait_recv()
        summed = summed + cr[rel * 4 + d]
    p1 = x * other + y * c
    p2 = x * c + y * other
    g_own[p2, p1, 0] = (total + summed).astype(BF16)

    def d1(o):
        return remote(g_own.at[p2, p1, 0], g_own.at[p2, p1, o], d1_send.at[o], d1_recv.at[o], (at_z(-NEAR[o]), c, x, y))

    for o in reversed(range(1, NZ)):
        go(d1(o))

    def along_first(d):
        return (z, c, ring4(x, d * other), ring4(y, d * c))

    def along_second(d):
        return (z, c, ring4(x, d * c), ring4(y, d * other))

    SIDE = {1: 0, 3: 1, 2: 2}

    def whole(s):
        return pl.ds(s * CHUNK, CHUNK)

    def half(s, n):
        return pl.ds(s * CHUNK + n * (CHUNK // 2), CHUNK // 2)

    def first(slab, i, d):
        return remote(slab, slab, d2_send.at[i], d2_recv.at[i], along_first(d))

    def second(slab, i, d):
        return remote(slab, slab, d3_send.at[i], d3_recv.at[i], along_second(d))

    def slab1(e, part):
        return g_own.at[p2, ring4(p1, (4 - e) % 4), part]

    def slab2(d, e, part):
        return g_own.at[ring4(p2, (4 - d) % 4), ring4(p1, (4 - e) % 4), part]

    def straight(send, part, base):
        for d in ORDER:
            if d == 2 and MODE == 2 and part < LAST:
                send(half(part, 0), base + 2, 2)
            else:
                send(whole(part), base + SIDE[d], d)

    def send_first(s):
        straight(lambda lines, i, d: go(first(slab1(0, lines), i, d)), s, s * 4)

    def send_second(s, e):
        straight(lambda lines, i, d: go(second(slab1(e, lines), i, d)), s, (s * 4 + e) * 4)

    def on_first(s, e):
        if e == 2 and MODE == 2 and s < LAST:
            for n in range(2):
                first(slab1(2, half(s, n)), s * 4 + 2 + n, 1).wait_recv()
        else:
            first(slab1(e, whole(s)), s * 4 + SIDE[e], 1).wait_recv()
            if e == 3 and MODE == 2 and s < LAST:
                go(first(slab1(e, half(s, 1)), s * 4 + 3, e))
        send_second(s, e)

    def on_second(s, e, d):
        base = (s * 4 + e) * 4
        if d == 2 and MODE == 2 and s < LAST:
            for n in range(2):
                second(slab2(2, e, half(s, n)), base + 2 + n, 1).wait_recv()
        else:
            second(slab2(d, e, whole(s)), base + SIDE[d], 1).wait_recv()
            if d == 3 and MODE == 2 and s < LAST:
                go(second(slab2(d, e, half(s, 1)), base + 3, d))

    def on_origin(s):
        for o in range(max(1, s * CHUNK), (s + 1) * CHUNK):
            d1(o).wait_recv()
        send_first(s)
        send_second(s, 0)

    def held(core_rows, parity, n):
        xx, yy = n % 4, 2 * core_rows + n // 4
        return xx * parity + yy * (1 - parity), xx * (1 - parity) + yy * parity

    def d4(s, n, rows, parity, src, dst):
        i, j = held(rows, parity, n)
        k = s * 8 + n
        return remote(src.at[i, j, whole(s)], dst.at[i, j, whole(s)], d4_send.at[k], d4_recv.at[k], (z, other, x, y))

    def squares(ref, s, rows, parity, n):
        i, j = held(rows, parity, n)
        part = ref[i, j, s * CHUNK : (s + 1) * CHUNK].astype(F32)
        return jnp.sum(part * part, 0)

    def on_complete(s):
        for n in range(8):
            go(d4(s, n, other, c, g_own, g_other))
        for n in range(8):
            found = squares(g_own, s, c, c, n)
            rb[n] = found if s == 0 else rb[n] + found

    for s in range(CHUNKS):
        on_origin(s)
    for s in range(CHUNKS):
        for e in (1, 3, 2):
            on_first(s, e)
    for s in range(CHUNKS):
        for e in (0, 1, 3, 2):
            for d in (1, 3, 2):
                on_second(s, e, d)
        on_complete(s)

    for s in range(CHUNKS):
        for n in range(8):
            d4(s, n, c, other, g_other, g_other).wait_recv()
            rb[n] = rb[n] + squares(g_other, s, c, other, n)
    for n in range(8):
        total_sq = jnp.sum(rb[n], -1, keepdims=True)
        rb[n] = jnp.broadcast_to(lax.rsqrt(total_sq * (1.0 / 4096) + 1e-05), (32, 128))

    loads[3].wait()
    lm_copy_in = remote(lm_hbm, lm_buf.at[other], b_send.at[1], b_recv.at[1], (z, other, x, y))
    lm_copy_in.wait_recv()
    for o in range(NZ):
        for ref, parity in ((g_own, c), (g_other, other)):
            at = pl.multiple_of((at_z(NEAR[o]) * 2 + parity) * 128, 128)
            gain = gain_ref[:, pl.ds(at, 128)]
            for n in range(8):
                i, j = held(c, parity, n)
                tile = (ref[i, j, o].astype(F32) * rb[n] * gain).astype(BF16)
                normed[o, n * 32 : (n + 1) * 32, pl.ds(pl.multiple_of(parity * 128, 128), 128)] = tile
        if o % 2:
            for part in range(2):
                grown = 0.0 if o == 1 else acc[part]
                for k in (o - 1, o):
                    lanes = pl.ds(pl.multiple_of(at_z(NEAR[k]) * 256, 256), 256)
                    grown = grown + nt_dot(lm_buf[part, :, lanes], normed[k])
                acc[part] = grown

    logits = [acc[0], acc[1]]
    peak = jnp.maximum(jnp.max(logits[0], 0, keepdims=True), jnp.max(logits[1], 0, keepdims=True))
    wanted = jnp.concatenate([tgt_ref[pl.ds(2 * c, 1), :], tgt_ref[pl.ds(2 * c + 1, 1), :]], 1)
    spread = jnp.zeros((1, 256), F32)
    picked = jnp.zeros((1, 256), F32)
    for half in range(2):
        base = (((2 * z + half) * NX + x) * NY + y) * 256
        entry = base + lax.broadcasted_iota(jnp.int32, (256, 256), 0)
        spread += jnp.sum(jnp.exp(logits[half] - peak), 0, keepdims=True)
        picked += jnp.sum(jnp.where(entry == wanted, logits[half], 0.0), 0, keepdims=True)
    partial = peak + jnp.log(spread)
    for n in range(2):
        st[n, 0:1] = partial[:, n * 128 : (n + 1) * 128]
        st[n, 1:2] = picked[:, n * 128 : (n + 1) * 128]

    active = c == y // 2

    def f1(n, d, e):
        i = d * 4 + e
        return remote(st.at[n], fr.at[x * 4 + y], f1_send.at[n * 4 + d], f1_recv.at[i], (z, c, ring4(x, d), 2 * c + n))

    for n in range(2):
        e = lax.rem(2 * c + n - y + 4, 4)
        for d in (2, 1, 3):
            f1(n, d, e).start()

        @pl.when(e != 0)
        def _():
            f1(n, 0, e).start()

        @pl.when(e == 0)
        def _():
            fr[x * 4 + y] = st[n]

    def joined(ref):
        heads = [ref[n] for n in range(16)]
        high = functools.reduce(jnp.maximum, [part[0:1] for part in heads])
        mass = functools.reduce(jnp.add, [jnp.exp(part[0:1] - high) for part in heads])
        return high + jnp.log(mass), functools.reduce(jnp.add, [part[1:2] for part in heads])

    def f2(o, core, n):
        return remote(fs, zr.at[o], f2_send.at[2 * o + n], f2_recv.at[o], (at_z(-NEAR[o]), core, x, y))

    @pl.when(active)
    def _():
        for d in range(4):
            for e in range(4):
                if d or e:
                    here = fr.at[lax.rem(x + 4 - d, 4) * 4 + lax.rem(y + 4 - e, 4)]
                    remote(st.at[0], here, f1_send.at[0], f1_recv.at[d * 4 + e], (z, c, x, y)).wait_recv()
        level, hit = joined(fr)
        fs[0:1] = level
        fs[1:2] = hit
        for o in reversed(range(1, NZ)):
            f2(o, c, 0).start()
            f2(o, other, 1).start()
        f2(0, other, 1).start()
        zr[0] = fs[...]

    for o in range(1, NZ):
        f2(o, c, 0).wait_recv()

    @pl.when(jnp.logical_not(active))
    def _():
        f2(0, other, 1).wait_recv()

    level, hit = joined(zr)
    logprob = hit - level
    spots = lax.broadcasted_iota(jnp.int32, (1, 128), 1) * 64 + 31
    count = jnp.zeros((1, 1), F32)
    for n in range(4):
        count += jnp.sum(jnp.where(spots < len_ref[n], 1.0, 0.0), -1, keepdims=True)
    mine = jnp.where(spots < len_ref[y], 1.0, 0.0)
    score = jnp.sum(mine * logprob, -1, keepdims=True) / count
    out_ref[0:1] = logprob
    out_ref[1:2] = jnp.broadcast_to(score, (1, 128))

    for copy in sent:
        copy.wait_send()
    for n in range(2):
        e = lax.rem(2 * c + n - y + 4, 4)
        for d in (2, 1, 3):
            f1(n, d, e).wait_send()

        @pl.when(e != 0)
        def _():
            f1(n, 0, e).wait_send()

    @pl.when(active)
    def _():
        for o in reversed(range(1, NZ)):
            f2(o, c, 0).wait_send()
            f2(o, other, 1).wait_send()
        f2(0, other, 1).wait_send()


def body(
    queries, keys, values, key_position, compress_keys, compress_values,
    out_proj, residual, norm_gain, lm_head, targets, lengths,
):
    vmem = pl.BlockSpec(memory_space=pltpu.VMEM)
    hbm = pl.BlockSpec(memory_space=pltpu.HBM)
    dma = pltpu.SemaphoreType.DMA
    found = pl.pallas_call(
        kernel,
        out_shape=jax.ShapeDtypeStruct((2, 128), F32),
        in_specs=[hbm] * 12,
        out_specs=vmem,
        scratch_shapes=[
            pltpu.VMEM((1, 4, 1024), BF16),
            pltpu.VMEM((1, 256, 256), BF16),
            pltpu.VMEM((1, 256, 256), BF16),
            pltpu.VMEM((32, 128), F32),
            pltpu.VMEM((4, 128, 128), BF16),
            pltpu.VMEM((1, 4096), F32),
            pltpu.VMEM((4, 128), jnp.int32),
            pltpu.SMEM((4,), jnp.int32),
            pltpu.VMEM((2, 4096, 128), BF16),
            pltpu.VMEM((512, 128), BF16),
            pltpu.VMEM((512, 128), BF16),
            pltpu.VMEM((2, 256, 4096), BF16),
            pltpu.VMEM((2, 2, 256, 128), F32),
            pltpu.VMEM((2, 32, 2048), BF16),
            pltpu.VMEM((2, 48, 2048), BF16),
            pltpu.VMEM((2, 3, 16, 128), BF16),
            pltpu.VMEM((2, 4, 128), F32),
            pltpu.VMEM((2, 1, 128), F32),
            pltpu.VMEM((16, 2, 3, 16, 128), BF16),
            pltpu.VMEM((16, 2, 4, 128), F32),
            pltpu.VMEM((512, 128), BF16),
            pltpu.VMEM((512, 128), BF16),
            pltpu.VMEM((512, 128), BF16),
            pltpu.VMEM((128, 512), BF16),
            pltpu.VMEM((2, 4, 32, 128), F32),
            pltpu.VMEM((8, 32, 128), F32),
            pltpu.VMEM((4, 4, 16, 32, 128), BF16),
            pltpu.VMEM((4, 4, 16, 32, 128), BF16),
            pltpu.VMEM((8, 32, 128), F32),
            pltpu.VMEM((16, 256, 256), BF16),
            pltpu.VMEM((2, 256, 256), F32),
            pltpu.VMEM((2, 2, 128), F32),
            pltpu.VMEM((16, 2, 128), F32),
            pltpu.VMEM((2, 128), F32),
            pltpu.VMEM((16, 2, 128), F32),
            dma((4,)), dma((8,)),
            dma((2,)), dma((2,)),
            dma((28,)), dma((28,)),
            dma((12,)), dma((12,)),
            dma((8,)), dma((8,)),
            dma((16,)), dma((16,)),
            dma((16,)), dma((16,)),
            dma((64,)), dma((64,)),
            dma((32,)), dma((32,)),
            dma((8,)), dma((16,)),
            dma((32,)), dma((16,)),
        ],
        compiler_params=pltpu.CompilerParams(
            collective_id=0, has_side_effects=True, vmem_limit_bytes=67043328
        ),
    )(
        queries, keys, values, key_position, compress_keys, compress_values,
        out_proj, residual, norm_gain.reshape(1, -1), lm_head, targets, lengths,
    )
    seq_pos = lax.axis_index(SEQ)
    token_logprob = lax.dynamic_slice(found, (0, seq_pos * 4), (1, 4))
    return token_logprob, found[1, :1]


def solution(mesh):
    split = Mesh(
        mesh.devices.reshape(16, 2, mesh.shape["mp"], mesh.shape["batch"]),
        ("seq_0", "seq_1", "mp", "batch"),
    )
    in_specs = (
        P("batch", SEQ, "mp"),
        P("batch", SEQ, "mp"),
        P("batch", SEQ, "mp"),
        P(),
        P(),
        P(),
        P("mp", SEQ),
        P(None, None, SEQ),
        P(),
        P(SEQ_MP_BATCH, None),
        P(),
        P(),
    )
    out_specs = (P("batch", SEQ), P("batch"))
    return jax.shard_map(body, mesh=split, in_specs=in_specs, out_specs=out_specs, check_vma=False)
```

```python
import functools
import math

import jax
import jax.numpy as jnp
from jax import lax
from jax.experimental import pallas as pl
from jax.experimental.pallas import tpu as pltpu
from jax.sharding import Mesh
from jax.sharding import PartitionSpec as P

BF16 = jnp.bfloat16
F32 = jnp.float32
HEAD_DIM = 128
MESH = pl.DeviceIdType.MESH
AXES = ("seq_0", "seq_1", "mp", "batch")
SEQ = ("seq_0", "seq_1")
SEQ_MP_BATCH = ("seq_0", "seq_1", "mp", "batch")
NZ, NX, NY = 16, 4, 4

SHIFT = (0, 1, 2, -1, -2)
STEP = (0, 5, -5)
OFFSETS = tuple(s + w for s in SHIFT for w in STEP) + (8,)
ROUND_ONE = (1, 2, 6, 12, 3, 9, 0)
SLOT_OF = {off % NZ: k for k, off in enumerate(OFFSETS)}
NEAR = (0, 1, -1, 2, -2, 3, -3, 4, -4, 5, -5, 6, -6, 7, -7, 8)
CHUNK = 4
MODE = 0
ORDER = (1, 3, 2)
CHUNKS = NZ // CHUNK
LAST = CHUNKS - 1


def nt_dot(a, b):
    return lax.dot_general(a, b, (((1,), (1,)), ((), ())), preferred_element_type=F32)


def kernel(
    q_hbm, k_hbm, v_hbm, pos_hbm, wk_hbm, wv_hbm, op_hbm, res_hbm, gain_hbm, lm_hbm, tgt_hbm, len_hbm,
    out_ref,
    q_ref, k_ref, v_ref, pos_ref, res_ref, gain_ref, tgt_ref, len_ref, w_buf, op_own, op_other, lm_buf, rows_f, xa, xb, pay, epay, bz, kvq, ebuf, qperm, kmat, vmat, att,
    cs, cr, g_own, g_other, rb, normed, acc, st, fr, fs, zr,
    local_sem, small_sem, b_send, b_recv, a1_send, a1_recv, a2_send, a2_recv, c_send, c_recv, d1_send, d1_recv,
    d2_send, d2_recv, d3_send, d3_recv, d4_send, d4_recv, f1_send, f1_recv, f2_send, f2_recv,
):
    z, c, x, y = (lax.axis_index(name) for name in AXES)
    other = 1 - c

    def at_z(off):
        return lax.rem(z + (off + NZ), NZ)

    def ring4(p, d):
        return lax.rem(p + d, 4)

    barrier = pltpu.get_barrier_semaphore()
    peers = [(at_z(off), core, x, y) for off in range(1, NZ) for core in (0, 1)]
    peers += [(z, other, ring4(x, d), y) for d in range(4)]
    peers += [(z, c, ring4(x, d), ring4(y, e)) for d in range(4) for e in range(4) if d or e]
    loads = [
        pltpu.make_async_copy(wk_hbm, w_buf.at[0], local_sem.at[0]),
        pltpu.make_async_copy(wv_hbm, w_buf.at[1], local_sem.at[1]),
        pltpu.make_async_copy(op_hbm.at[pl.ds(pl.multiple_of(c * 512, 512), 512)], op_own, local_sem.at[2]),
        pltpu.make_async_copy(lm_hbm, lm_buf.at[c], local_sem.at[3]),
    ]
    small = [
        pltpu.make_async_copy(src, dst, small_sem.at[n])
        for n, (src, dst) in enumerate((
            (k_hbm, k_ref), (v_hbm, v_ref), (pos_hbm, pos_ref), (q_hbm, q_ref),
            (res_hbm, res_ref), (gain_hbm, gain_ref), (tgt_hbm, tgt_ref), (len_hbm, len_ref),
        ))
    ]
    for load in small[:4] + loads[:2]:
        load.start()
    for peer in peers:
        pl.semaphore_signal(barrier, inc=1, device_id=peer, device_id_type=MESH)
    for load in loads[2:] + small[4:]:
        load.start()
    for load in small[:4]:
        load.wait()

    for t, src in enumerate((k_ref, v_ref)):
        for h in range(2):
            rows_f[t, h] = src[0, :, h * 128 : (h + 1) * 128].astype(F32)
    for i in range(16):
        lanes = slice(i * 128, (i + 1) * 128)
        pa, pb = pos_ref[i : i + 1, :], pos_ref[16 + i : 17 + i, :]
        for t in range(2):
            for h in range(2):
                rows = rows_f[t, h, pl.ds(i, 16, stride=16), :]
                xa[t, h * 16 : (h + 1) * 16, lanes] = (rows + pa).astype(BF16)
                xb[t, h * 16 : (h + 1) * 16, lanes] = (rows + pb).astype(BF16)
            xb[t, 32:48, lanes] = jnp.broadcast_to(pb, (16, 128)).astype(BF16)
    qf = q_ref[0].astype(F32)
    for h in range(2):
        lines = [qf[:, (4 * h + g) * 128 : (4 * h + g + 1) * 128] for g in range(4)]
        pay[h, 2] = jnp.concatenate(lines, 0).astype(BF16)
    for t in range(2):
        loads[t].wait()
        first = jnp.dot(xa[t], w_buf[t, :2048], preferred_element_type=F32)
        second = jnp.dot(xb[t], w_buf[t, 2048:], preferred_element_type=F32)
        bz[t] = second[32:33]
        for h in range(2):
            fh, sh = first[h * 16 : (h + 1) * 16], second[h * 16 : (h + 1) * 16]
            pay[h, t] = (fh + pltpu.roll(sh, 15, 0)).astype(BF16)
            epay[h, 2 * t : 2 * t + 1] = fh[15:16]
            epay[h, 2 * t + 1 : 2 * t + 2] = sh[0:1]
    kvq[0, c] = pay[c]
    ebuf[0, c] = epay[c]

    pl.semaphore_wait(barrier, len(peers))

    def remote(src, dst, send, recv, peer):
        return pltpu.make_async_remote_copy(
            src_ref=src, dst_ref=dst, send_sem=send, recv_sem=recv, device_id=peer, device_id_type=MESH
        )

    sent = []

    def go(copy):
        copy.start()
        sent.append(copy)

    def a1(n, k, core, h):
        peer = (at_z(-OFFSETS[k]), core, x, y)
        i, j = 4 * ROUND_ONE.index(k) + 2 * n, 4 * ROUND_ONE.index(k) + 2 * c
        return (
            remote(pay.at[h], kvq.at[k, c], a1_send.at[i], a1_recv.at[j], peer),
            remote(epay.at[h], ebuf.at[k, c], a1_send.at[i + 1], a1_recv.at[j + 1], peer),
        )

    for k in ROUND_ONE[:-1]:
        for n, h in enumerate((c, other)):
            for part in a1(n, k, h, h):
                go(part)
    for part in a1(0, 0, other, other):
        go(part)

    op_copy = remote(op_hbm.at[pl.ds(pl.multiple_of(other * 512, 512), 512)], op_other, b_send.at[0], b_recv.at[0], (z, other, x, y))
    lm_copy = remote(lm_hbm, lm_buf.at[c], b_send.at[1], b_recv.at[1], (z, other, x, y))
    go(op_copy)
    go(lm_copy)

    def a1_arrival(k, core):
        j = 4 * ROUND_ONE.index(k) + 2 * core
        remote(pay.at[0], kvq.at[k, core], a1_send.at[0], a1_recv.at[j], (z, c, x, y)).wait_recv()
        remote(epay.at[0], ebuf.at[k, core], a1_send.at[0], a1_recv.at[j + 1], (z, c, x, y)).wait_recv()

    for k in (1, 2):
        for core in range(2):
            a1_arrival(k, core)

    def a2(g):
        peer = (at_z(-SHIFT[g]), c, x, y)
        src, dst, i = pl.ds(1, 2), pl.ds(3 * g + 1, 2), 2 * g - 2
        return (
            remote(kvq.at[src], kvq.at[dst], a2_send.at[i], a2_recv.at[i], peer),
            remote(ebuf.at[src], ebuf.at[dst], a2_send.at[i + 1], a2_recv.at[i + 1], peer),
        )

    def a2_far(n):
        peer = (at_z(-3 if n == 0 else 3), c, x, y)
        i = 8 + 2 * n
        return (
            remote(kvq.at[1 + n, n], kvq.at[15, n], a2_send.at[i], a2_recv.at[i], peer),
            remote(ebuf.at[1 + n, n], ebuf.at[15, n], a2_send.at[i + 1], a2_recv.at[i + 1], peer),
        )

    for n in (0, 1):
        for part in a2_far(n):
            go(part)
    for g in (2, 4, 1, 3):
        for part in a2(g):
            go(part)

    col = lax.broadcasted_iota(jnp.int32, (1, 512), 1)
    slot, core_of, lane = col // 32, (col // 16) % 2, col % 16
    g_of, w_of = slot // 3, slot % 3
    off_of = jnp.where(g_of > 2, 2 - g_of, g_of) + jnp.where(w_of == 2, -5, 5 * w_of)
    off_of = jnp.where(slot == 15, 8, off_of)
    seq_of = ((off_of + z + NZ) % NZ) * 2 + core_of
    block_of = seq_of * 16 + lane
    row_of = (lane // 4) * 128 + seq_of * 4 + lane % 4
    perm = jnp.where(lax.broadcasted_iota(jnp.int32, (512, 512), 0) == row_of, 1.0, 0.0).astype(BF16)

    a1_arrival(0, other)
    for k in (3, 9, 6, 12):
        for core in range(2):
            a1_arrival(k, core)
    for g in (1, 3, 2, 4):
        for part in a2(g):
            part.wait_recv()
    for n in (0, 1):
        for part in a2_far(n):
            part.wait_recv()

    q_all = kvq[:, :, 2].reshape(512, 128)
    qperm[...] = jnp.dot(perm, q_all, preferred_element_type=F32).astype(BF16)
    last = lax.broadcasted_iota(jnp.int32, (16, 128), 0) == 15
    for k in range(NZ):
        top = (at_z(OFFSETS[k]) == NZ - 1).astype(F32)
        after = SLOT_OF[(OFFSETS[k] + 1) % NZ]
        for t, mat in enumerate((kmat, vmat)):
            for core in range(2):
                if core == 0:
                    beyond = ebuf[k, 1, 2 * t + 1 : 2 * t + 2]
                else:
                    beyond = ebuf[after, 0, 2 * t + 1 : 2 * t + 2] * (1.0 - top) + bz[t] * top
                fixed = ebuf[k, core, 2 * t : 2 * t + 1] + beyond
                tile = jnp.where(last, fixed, kvq[k, core, t].astype(F32))
                mat[(2 * k + core) * 16 : (2 * k + core + 1) * 16, :] = tile.astype(BF16)

    limit = lax.broadcasted_iota(jnp.int32, (128, 1), 0) * 4
    visible = block_of <= limit
    for g in range(4):
        score = nt_dot(qperm[g * 128 : (g + 1) * 128], kmat[...]) * (1.0 / math.sqrt(HEAD_DIM))
        score = jnp.where(visible, score, -1e30)
        peak = jnp.max(score, -1, keepdims=True)
        weight = jnp.where(visible, jnp.exp(score - peak), 0.0)
        prob = (weight * (1.0 / jnp.sum(weight, -1, keepdims=True))).astype(BF16)
        found = jnp.dot(prob, vmat[...], preferred_element_type=F32)
        att[:, g * 128 : (g + 1) * 128] = found.astype(BF16)

    loads[2].wait()
    cs[0] = jnp.dot(att[...], op_own[...], preferred_element_type=F32).reshape(4, 32, 128)
    op_copy.wait_recv()
    cs[1] = jnp.dot(att[...], op_other[...], preferred_element_type=F32).reshape(4, 32, 128)

    def c_copy(rel, d):
        to = ring4(x, d)
        i = rel * 4 + d
        return remote(cs.at[rel, to], cr.at[i], c_send.at[i], c_recv.at[i], (z, other if rel else c, to, y))

    pairs = [(rel, d) for d in (2, 1, 3, 0) for rel in (0, 1) if rel or d]
    for rel, d in pairs:
        go(c_copy(rel, d))
    for load in small[4:]:
        load.wait()
    total = res_ref[y, pl.ds(pl.multiple_of(32 * x, 32), 32), :].astype(F32)
    summed = cs[0, x]
    for rel, d in reversed(pairs):
        c_copy(rel, d).wait_recv()
        summed = summed + cr[rel * 4 + d]
    p1 = x * other + y * c
    p2 = x * c + y * other
    g_own[p2, p1, 0] = (total + summed).astype(BF16)

    def d1(o):
        return remote(g_own.at[p2, p1, 0], g_own.at[p2, p1, o], d1_send.at[o], d1_recv.at[o], (at_z(-NEAR[o]), c, x, y))

    for o in reversed(range(1, NZ)):
        go(d1(o))

    def along_first(d):
        return (z, c, ring4(x, d * other), ring4(y, d * c))

    def along_second(d):
        return (z, c, ring4(x, d * c), ring4(y, d * other))

    SIDE = {1: 0, 3: 1, 2: 2}

    def whole(s):
        return pl.ds(s * CHUNK, CHUNK)

    def half(s, n):
        return pl.ds(s * CHUNK + n * (CHUNK // 2), CHUNK // 2)

    def first(slab, i, d):
        return remote(slab, slab, d2_send.at[i], d2_recv.at[i], along_first(d))

    def second(slab, i, d):
        return remote(slab, slab, d3_send.at[i], d3_recv.at[i], along_second(d))

    def slab1(e, part):
        return g_own.at[p2, ring4(p1, (4 - e) % 4), part]

    def slab2(d, e, part):
        return g_own.at[ring4(p2, (4 - d) % 4), ring4(p1, (4 - e) % 4), part]

    def straight(send, part, base):
        for d in ORDER:
            if d == 2 and MODE == 2 and part < LAST:
                send(half(part, 0), base + 2, 2)
            else:
                send(whole(part), base + SIDE[d], d)

    def send_first(s):
        straight(lambda lines, i, d: go(first(slab1(0, lines), i, d)), s, s * 4)

    def send_second(s, e):
        straight(lambda lines, i, d: go(second(slab1(e, lines), i, d)), s, (s * 4 + e) * 4)

    def on_first(s, e):
        if e == 2 and MODE == 2 and s < LAST:
            for n in range(2):
                first(slab1(2, half(s, n)), s * 4 + 2 + n, 1).wait_recv()
        else:
            first(slab1(e, whole(s)), s * 4 + SIDE[e], 1).wait_recv()
            if e == 3 and MODE == 2 and s < LAST:
                go(first(slab1(e, half(s, 1)), s * 4 + 3, e))
        send_second(s, e)

    def on_second(s, e, d):
        base = (s * 4 + e) * 4
        if d == 2 and MODE == 2 and s < LAST:
            for n in range(2):
                second(slab2(2, e, half(s, n)), base + 2 + n, 1).wait_recv()
        else:
            second(slab2(d, e, whole(s)), base + SIDE[d], 1).wait_recv()
            if d == 3 and MODE == 2 and s < LAST:
                go(second(slab2(d, e, half(s, 1)), base + 3, d))

    def on_origin(s):
        for o in range(max(1, s * CHUNK), (s + 1) * CHUNK):
            d1(o).wait_recv()
        send_first(s)
        send_second(s, 0)

    def held(core_rows, parity, n):
        xx, yy = n % 4, 2 * core_rows + n // 4
        return xx * parity + yy * (1 - parity), xx * (1 - parity) + yy * parity

    def d4(s, n, rows, parity, src, dst):
        i, j = held(rows, parity, n)
        k = s * 8 + n
        return remote(src.at[i, j, whole(s)], dst.at[i, j, whole(s)], d4_send.at[k], d4_recv.at[k], (z, other, x, y))

    def squares(ref, s, rows, parity, n):
        i, j = held(rows, parity, n)
        part = ref[i, j, s * CHUNK : (s + 1) * CHUNK].astype(F32)
        return jnp.sum(part * part, 0)

    def on_complete(s):
        for n in range(8):
            go(d4(s, n, other, c, g_own, g_other))
        for n in range(8):
            found = squares(g_own, s, c, c, n)
            rb[n] = found if s == 0 else rb[n] + found

    for s in range(CHUNKS):
        on_origin(s)
    for s in range(CHUNKS):
        for e in (1, 3, 2):
            on_first(s, e)
    for s in range(CHUNKS):
        for e in (0, 1, 3, 2):
            for d in (1, 3, 2):
                on_second(s, e, d)
        on_complete(s)

    for s in range(CHUNKS):
        for n in range(8):
            d4(s, n, c, other, g_other, g_other).wait_recv()
            rb[n] = rb[n] + squares(g_other, s, c, other, n)
    for n in range(8):
        total_sq = jnp.sum(rb[n], -1, keepdims=True)
        rb[n] = jnp.broadcast_to(lax.rsqrt(total_sq * (1.0 / 4096) + 1e-05), (32, 128))

    loads[3].wait()
    lm_copy_in = remote(lm_hbm, lm_buf.at[other], b_send.at[1], b_recv.at[1], (z, other, x, y))
    lm_copy_in.wait_recv()
    for o in range(NZ):
        for ref, parity in ((g_own, c), (g_other, other)):
            at = pl.multiple_of((at_z(NEAR[o]) * 2 + parity) * 128, 128)
            gain = gain_ref[:, pl.ds(at, 128)]
            for n in range(8):
                i, j = held(c, parity, n)
                tile = (ref[i, j, o].astype(F32) * rb[n] * gain).astype(BF16)
                normed[o, n * 32 : (n + 1) * 32, pl.ds(pl.multiple_of(parity * 128, 128), 128)] = tile
        if o % 2:
            for part in range(2):
                grown = 0.0 if o == 1 else acc[part]
                for k in (o - 1, o):
                    lanes = pl.ds(pl.multiple_of(at_z(NEAR[k]) * 256, 256), 256)
                    grown = grown + nt_dot(lm_buf[part, :, lanes], normed[k])
                acc[part] = grown

    logits = [acc[0], acc[1]]
    peak = jnp.maximum(jnp.max(logits[0], 0, keepdims=True), jnp.max(logits[1], 0, keepdims=True))
    wanted = jnp.concatenate([tgt_ref[pl.ds(2 * c, 1), :], tgt_ref[pl.ds(2 * c + 1, 1), :]], 1)
    spread = jnp.zeros((1, 256), F32)
    picked = jnp.zeros((1, 256), F32)
    for half in range(2):
        base = (((2 * z + half) * NX + x) * NY + y) * 256
        entry = base + lax.broadcasted_iota(jnp.int32, (256, 256), 0)
        spread += jnp.sum(jnp.exp(logits[half] - peak), 0, keepdims=True)
        picked += jnp.sum(jnp.where(entry == wanted, logits[half], 0.0), 0, keepdims=True)
    partial = peak + jnp.log(spread)
    for n in range(2):
        st[n, 0:1] = partial[:, n * 128 : (n + 1) * 128]
        st[n, 1:2] = picked[:, n * 128 : (n + 1) * 128]

    active = c == y // 2

    def f1(n, d, e):
        i = d * 4 + e
        return remote(st.at[n], fr.at[x * 4 + y], f1_send.at[n * 4 + d], f1_recv.at[i], (z, c, ring4(x, d), 2 * c + n))

    for n in range(2):
        e = lax.rem(2 * c + n - y + 4, 4)
        for d in (2, 1, 3):
            f1(n, d, e).start()

        @pl.when(e != 0)
        def _():
            f1(n, 0, e).start()

        @pl.when(e == 0)
        def _():
            fr[x * 4 + y] = st[n]

    def joined(ref):
        heads = [ref[n] for n in range(16)]
        high = functools.reduce(jnp.maximum, [part[0:1] for part in heads])
        mass = functools.reduce(jnp.add, [jnp.exp(part[0:1] - high) for part in heads])
        return high + jnp.log(mass), functools.reduce(jnp.add, [part[1:2] for part in heads])

    def f2(o, core, n):
        return remote(fs, zr.at[o], f2_send.at[2 * o + n], f2_recv.at[o], (at_z(-NEAR[o]), core, x, y))

    @pl.when(active)
    def _():
        for d in range(4):
            for e in range(4):
                if d or e:
                    here = fr.at[lax.rem(x + 4 - d, 4) * 4 + lax.rem(y + 4 - e, 4)]
                    remote(st.at[0], here, f1_send.at[0], f1_recv.at[d * 4 + e], (z, c, x, y)).wait_recv()
        level, hit = joined(fr)
        fs[0:1] = level
        fs[1:2] = hit
        for o in reversed(range(1, NZ)):
            f2(o, c, 0).start()
            f2(o, other, 1).start()
        f2(0, other, 1).start()
        zr[0] = fs[...]

    for copy in sent:
        copy.wait_send()

    for o in range(1, NZ):
        f2(o, c, 0).wait_recv()

    @pl.when(jnp.logical_not(active))
    def _():
        f2(0, other, 1).wait_recv()

    level, hit = joined(zr)
    logprob = hit - level
    spots = lax.broadcasted_iota(jnp.int32, (1, 128), 1) * 64 + 31
    count = jnp.zeros((1, 1), F32)
    for n in range(4):
        count += jnp.sum(jnp.where(spots < len_ref[n], 1.0, 0.0), -1, keepdims=True)
    mine = jnp.where(spots < len_ref[y], 1.0, 0.0)
    score = jnp.sum(mine * logprob, -1, keepdims=True) / count
    out_ref[0:1] = logprob
    out_ref[1:2] = jnp.broadcast_to(score, (1, 128))

    for n in range(2):
        e = lax.rem(2 * c + n - y + 4, 4)
        for d in (2, 1, 3):
            f1(n, d, e).wait_send()

        @pl.when(e != 0)
        def _():
            f1(n, 0, e).wait_send()

    @pl.when(active)
    def _():
        for o in reversed(range(1, NZ)):
            f2(o, c, 0).wait_send()
            f2(o, other, 1).wait_send()
        f2(0, other, 1).wait_send()


def body(
    queries, keys, values, key_position, compress_keys, compress_values,
    out_proj, residual, norm_gain, lm_head, targets, lengths,
):
    vmem = pl.BlockSpec(memory_space=pltpu.VMEM)
    hbm = pl.BlockSpec(memory_space=pltpu.HBM)
    dma = pltpu.SemaphoreType.DMA
    found = pl.pallas_call(
        kernel,
        out_shape=jax.ShapeDtypeStruct((2, 128), F32),
        in_specs=[hbm] * 12,
        out_specs=vmem,
        scratch_shapes=[
            pltpu.VMEM((1, 4, 1024), BF16),
            pltpu.VMEM((1, 256, 256), BF16),
            pltpu.VMEM((1, 256, 256), BF16),
            pltpu.VMEM((32, 128), F32),
            pltpu.VMEM((4, 128, 128), BF16),
            pltpu.VMEM((1, 4096), F32),
            pltpu.VMEM((4, 128), jnp.int32),
            pltpu.SMEM((4,), jnp.int32),
            pltpu.VMEM((2, 4096, 128), BF16),
            pltpu.VMEM((512, 128), BF16),
            pltpu.VMEM((512, 128), BF16),
            pltpu.VMEM((2, 256, 4096), BF16),
            pltpu.VMEM((2, 2, 256, 128), F32),
            pltpu.VMEM((2, 32, 2048), BF16),
            pltpu.VMEM((2, 48, 2048), BF16),
            pltpu.VMEM((2, 3, 16, 128), BF16),
            pltpu.VMEM((2, 4, 128), F32),
            pltpu.VMEM((2, 1, 128), F32),
            pltpu.VMEM((16, 2, 3, 16, 128), BF16),
            pltpu.VMEM((16, 2, 4, 128), F32),
            pltpu.VMEM((512, 128), BF16),
            pltpu.VMEM((512, 128), BF16),
            pltpu.VMEM((512, 128), BF16),
            pltpu.VMEM((128, 512), BF16),
            pltpu.VMEM((2, 4, 32, 128), F32),
            pltpu.VMEM((8, 32, 128), F32),
            pltpu.VMEM((4, 4, 16, 32, 128), BF16),
            pltpu.VMEM((4, 4, 16, 32, 128), BF16),
            pltpu.VMEM((8, 32, 128), F32),
            pltpu.VMEM((16, 256, 256), BF16),
            pltpu.VMEM((2, 256, 256), F32),
            pltpu.VMEM((2, 2, 128), F32),
            pltpu.VMEM((16, 2, 128), F32),
            pltpu.VMEM((2, 128), F32),
            pltpu.VMEM((16, 2, 128), F32),
            dma((4,)), dma((8,)),
            dma((2,)), dma((2,)),
            dma((28,)), dma((28,)),
            dma((12,)), dma((12,)),
            dma((8,)), dma((8,)),
            dma((16,)), dma((16,)),
            dma((16,)), dma((16,)),
            dma((64,)), dma((64,)),
            dma((32,)), dma((32,)),
            dma((8,)), dma((16,)),
            dma((32,)), dma((16,)),
        ],
        compiler_params=pltpu.CompilerParams(
            collective_id=0, has_side_effects=True, vmem_limit_bytes=67043328
        ),
    )(
        queries, keys, values, key_position, compress_keys, compress_values,
        out_proj, residual, norm_gain.reshape(1, -1), lm_head, targets, lengths,
    )
    seq_pos = lax.axis_index(SEQ)
    token_logprob = lax.dynamic_slice(found, (0, seq_pos * 4), (1, 4))
    return token_logprob, found[1, :1]


def solution(mesh):
    split = Mesh(
        mesh.devices.reshape(16, 2, mesh.shape["mp"], mesh.shape["batch"]),
        ("seq_0", "seq_1", "mp", "batch"),
    )
    in_specs = (
        P("batch", SEQ, "mp"),
        P("batch", SEQ, "mp"),
        P("batch", SEQ, "mp"),
        P(),
        P(),
        P(),
        P("mp", SEQ),
        P(None, None, SEQ),
        P(),
        P(SEQ_MP_BATCH, None),
        P(),
        P(),
    )
    out_specs = (P("batch", SEQ), P("batch"))
    return jax.shard_map(body, mesh=split, in_specs=in_specs, out_specs=out_specs, check_vma=False)
```
